128 devices in a mesh: area: 16 (over z_lo, y, core), layer: 8 (over z_hi, x).
Axes of the slice: x: 4, y: 4, z: 4 (z_hi: 2, z_lo: 2; z = z_hi * 2 + z_lo), core: 2. Of those that a mesh axis runs over, the one named last changes fastest.
Arguments:
- permeability: float32 [32, 8192, 512], P('layer', 'area'), may hold values from 0.1 to 10
- mobility: float32 [32, 8192, 512], P('layer', 'area'), may hold values from 0.3 to 3
- thickness: float32 [32], P('layer'), may hold values from 0.5 to 2
- caprock: int32 [8192, 512], P('area'), may hold values from 0 to 15
- plume: int32 [8192, 512], P('area'), may hold values from 0 to 31
- storage: float32 [8192, 512], P('area'), may hold values from 3.2 to 32
- source: float32 [8192, 512], P('area'), may hold values from -384 to 384
- pressure_old: float32 [8192, 512], P('area'), may hold values from -6 to 6
Outputs:
- cell_pressure: float32 [32, 8192, 512], P('layer', 'area')
- flux_rows: float32 [32, 8192, 512], P('layer', 'area')
- flux_cols: float32 [32, 8192, 512], P('layer', 'area')
The draws below stay inside these ranges and needn't reach their ends.
Inputs may be any that keep to these rules, and one draw needn't show every extreme that they name: Layers above layer caprock of a column are sealed rock. CO2 fills the open layers above layer plume of a column; where plume <= caprock a column holds no CO2.
All inputs are finite; a program needn't handle non-finite values.
Results may differ from the reference program's by a relative error of at most 0.0003.
Values sent between devices are 32-bit elements; how exact they have to be, the bound alone decides.
A program may use at most 128 MiB of HBM per device.

```python
import math
import jax
import jax.numpy as jnp

NY = 512
SWEEPS = 3
NX = 8192
NZ = 32


def draw_source(key, part):
    rough_key = jax.random.fold_in(jax.random.fold_in(key, 11), 0)
    source_field = jax.random.truncated_normal(rough_key, -6.0, 6.0, (NX, NY), jnp.float32)
    return 2.0 * NZ * source_field


def with_ends(drawn, stream_key, low, largest):
    longest = drawn.shape.index(max(drawn.shape))
    spots = []
    for shift in (0, 1):
        where = [jax.random.randint(jax.random.fold_in(stream_key, axis), (), 0, length) for axis, length in enumerate(drawn.shape)]
        where[longest] = (where[longest] + shift) % drawn.shape[longest]
        spots.append(tuple(where))
    return drawn.at[spots[0]].set(low).at[spots[1]].set(largest)


def steps_of(own_key, shape, shards, low, high):
    factor_of = 1.0
    for dim, parts in shards:
        steps = jax.random.uniform(jax.random.fold_in(jax.random.fold_in(own_key, 6), dim), (parts,), jnp.float32, low / len(shards), high / len(shards))
        factor_of = factor_of * jnp.repeat(jnp.exp(steps), shape[dim] // parts).reshape((-1,) + (1,) * (len(shape) - 1 - dim))
    return factor_of


def normal_values(rng, extent, spread, reach, shards=(), kind=jnp.bfloat16):
    array = spread * jax.random.normal(rng, extent, jnp.float32)
    if shards:
        array = array * steps_of(rng, extent, shards, -0.22, 0.18)
    return jnp.clip(array, -reach, reach).astype(kind)


def setup_inputs(seed: int = 0) -> dict:
    key_list = jax.random.split(jax.random.key(seed), 9)
    permeability = jnp.clip(jnp.exp(math.log(10.0) - 4.6051702 * jax.random.uniform(key_list[0], (NZ, NX, NY), jnp.float32) ** steps_of(key_list[0], (NZ, NX, NY), ((0, 8), (1, 16)), -0.2, 0.2)), 0.1, 10.0)
    mobility = jnp.clip(jnp.exp(math.log(3.0) - 2.3025851 * jax.random.uniform(key_list[1], (NZ, NX, NY), jnp.float32) ** steps_of(key_list[1], (NZ, NX, NY), ((0, 8), (1, 16)), -0.2, 0.2)), 0.3, 3.0)
    thickness = jnp.clip(jnp.exp(math.log(2.0) - 1.3862944 * jax.random.uniform(key_list[2], (NZ,), jnp.float32) ** steps_of(key_list[2], (NZ,), ((0, 8),), -0.2, 0.2)), 0.5, 2.0)
    caprock = with_ends(jax.random.randint(key_list[3], (NX, NY), 0, NZ // 2), jax.random.fold_in(key_list[3], 1), 0, (NZ // 2) - 1).astype(jnp.int32)
    plume = with_ends(jax.random.randint(key_list[4], (NX, NY), 0, NZ), jax.random.fold_in(key_list[4], 1), 0, NZ - 1).astype(jnp.int32)
    storage = jnp.clip(jnp.exp(math.log(32.0) - 2.3025851 * jax.random.uniform(key_list[5], (NX, NY), jnp.float32) ** steps_of(key_list[5], (NX, NY), ((0, 16),), -0.2, 0.2)), 3.2, 32.0)
    source = draw_source(jax.random.fold_in(key_list[8], 71), 0)
    pressure_old = normal_values(key_list[7], (NX, NY), 1.0, 6.0, ((0, 16),), jnp.float32)
    return {"permeability": permeability, "mobility": mobility, "thickness": thickness, "caprock": caprock, "plume": plume, "storage": storage, "source": source, "pressure_old": pressure_old}


buoyancy_scale = 0.3
gravity_scale = 0.05
gas_density = 0.7
brine_density = 1.0


def harmonic(near_value, far_value):
    summed = near_value + far_value
    divisor = jnp.where(summed > 0, summed, 1.0)
    return 2.0 * near_value * far_value / divisor


def neighbours(padded, row_count):
    widened = jnp.pad(padded, ((0, 0), (1, 1)))
    return [widened[0:row_count, 1:-1], widened[2:row_count + 2, 1:-1],
            widened[1:row_count + 1, 0:-2], widened[1:row_count + 1, 2:]]


def prepare(summed_pad, storage, source, pressure_old):
    row_count = storage.shape[0]
    trans_pad = summed_pad[0]
    buoy_pad = summed_pad[1]
    drive_pad = buoyancy_scale * summed_pad[2]
    trans_faces = [harmonic(trans_pad[1:row_count + 1], neighbour) for neighbour in neighbours(trans_pad, row_count)]
    buoy_faces = [harmonic(buoy_pad[1:row_count + 1], neighbour) for neighbour in neighbours(buoy_pad, row_count)]
    drive_centre = drive_pad[1:row_count + 1]
    gravity_drive = sum(face_coef * (neighbour - drive_centre) for face_coef, neighbour in zip(buoy_faces, neighbours(drive_pad, row_count)))
    right_hand = storage * pressure_old + source + gravity_drive
    diagonal = storage + trans_faces[0] + trans_faces[1] + trans_faces[2] + trans_faces[3]
    return trans_faces, right_hand, diagonal


def relax(trans_faces, right_hand, diagonal, padded):
    row_count = right_hand.shape[0]
    inflow = sum(face_coef * neighbour for face_coef, neighbour in zip(trans_faces, neighbours(padded, row_count)))
    return (right_hand + inflow) / diagonal


def reference(permeability, mobility, thickness, caprock, plume, storage, source, pressure_old):
    layers = jnp.arange(NZ, dtype=jnp.int32)[:, None, None]
    open_cell = layers >= caprock[None]
    gas_cell = open_cell & (layers < plume[None])
    layer_thick = thickness[:, None, None]
    conduct = jnp.where(open_cell, permeability * mobility * layer_thick, 0.0)
    trans_col = jnp.sum(conduct, axis=0)
    buoy_col = jnp.sum(jnp.where(gas_cell, conduct, 0.0), axis=0)
    gas_height = jnp.sum(jnp.where(gas_cell, layer_thick, 0.0), axis=0)
    summed_pad = jnp.pad(jnp.stack([trans_col, buoy_col, gas_height]), ((0, 0), (1, 1), (0, 0)))
    trans_faces, right_hand, diagonal = prepare(summed_pad, storage, source, pressure_old)
    pressure = pressure_old
    for sweep_index in range(SWEEPS):
        pressure = relax(trans_faces, right_hand, diagonal, jnp.pad(pressure, ((1, 1), (0, 0))))
    layer_mass = layer_thick * jnp.where(gas_cell, gas_density, brine_density)
    hydro_head = jnp.cumsum(layer_mass, axis=0) - 0.5 * layer_mass
    cell_pressure = pressure[None] + gravity_scale * hydro_head
    next_conduct = jnp.pad(conduct[:, 1:, :], ((0, 0), (0, 1), (0, 0)))
    next_pressure = jnp.pad(cell_pressure[:, 1:, :], ((0, 0), (0, 1), (0, 0)))
    flux_rows = harmonic(conduct, next_conduct) * (cell_pressure - next_pressure)
    side_conduct = jnp.pad(conduct[:, :, 1:], ((0, 0), (0, 0), (0, 1)))
    side_pressure = jnp.pad(cell_pressure[:, :, 1:], ((0, 0), (0, 0), (0, 1)))
    flux_cols = harmonic(conduct, side_conduct) * (cell_pressure - side_pressure)
    return cell_pressure, flux_rows, flux_cols
```

```python
import functools

import jax
import jax.numpy as jnp
from jax import lax
from jax.experimental import pallas as pl
from jax.experimental.pallas import tpu as pltpu
from jax.sharding import PartitionSpec as P

SWEEPS = 3
buoyancy_scale = 0.3
gravity_scale = 0.05
gas_density = 0.7
brine_density = 1.0

LAYERS = 4
ROWS = 512
COLS = 512
SLAB = 64
HALO = 8
WIDE = SLAB + 2 * HALO
MESH = pl.DeviceIdType.MESH

ORDERS = ((0, 1, 2), (1, 2, 0), (2, 0, 1))
PART_START = (0, 24, 48)
PART_ROWS = (24, 24, 16)
FLIPS = ((1, 1, 1), (1, 1, 0), (0, 1, 1), (1, 0, 1), (1, 0, 0), (0, 1, 0), (0, 0, 1), (0, 0, 0))
OTHERS = FLIPS[:-1]


def harmonic(near_value, far_value):
    summed = near_value + far_value
    divisor = jnp.where(summed > 0, summed, 1.0)
    return 2.0 * near_value * far_value / divisor


def flip_of(*dims):
    return tuple(1 if d in dims else 0 for d in range(3))


class Place:
    def __init__(self):
        self.area = lax.axis_index("area")
        self.layer = lax.axis_index("layer")
        self.areas = lax.axis_size("area")
        x = self.layer % 4
        second = x // 2
        first = (x % 2) + second - 2 * (x % 2) * second
        self.code = (first, second, self.layer // 4)
        self.parity = self.area % 2
        self.slab = self.slab_of((0, 0, 0))

    def flipped(self, flip):
        return tuple((1 - c) if f else c for c, f in zip(self.code, flip))

    def layer_of(self, flip):
        first, second, half = self.flipped(flip)
        x = 2 * second + first + second - 2 * first * second
        return half * 4 + x

    def slab_of(self, flip):
        first, second, half = self.flipped(flip)
        x = 2 * second + first + second - 2 * first * second
        order = x + half * (7 - 2 * x)
        return order + self.parity * (7 - 2 * order)

    def layer_of_slab(self, slab):
        order = slab + self.parity * (7 - 2 * slab)
        return order + (order // 4) * (11 - 2 * order)

    def rows(self, flip, start, count):
        return pl.ds(pl.multiple_of(self.slab_of(flip) * SLAB + start, 8), count)


def gather_kernel(
    perm, mob, thick, cap, plu, sto, src, old,
    hh, hr, gr, hc, gc, pf,
    permv, mobv, cond, capv, pluv, tb, r1a, r1b, r1c, r2a, r2b, r2c, r3a, r3b, r3c,
    wide, edge_i, edge_f, thick_s, thick_all, table, gas, t_row, t_col, right_hand, inverse,
    in_sem, edge_sem, thick_sem, rs_send, rs_recv, ag_send, ag_recv, th_send, th_recv,
    halo_send, halo_recv, input_send, input_recv, row_send, row_recv, last_send, last_recv,
):
    here = Place()
    area, layer = here.area, here.layer
    r1, r2, r3 = (r1a, r1b, r1c), (r2a, r2b, r2c), (r3a, r3b, r3c)
    waits = []
    is_first = here.slab == 0
    is_last = here.slab == 7

    def peer(flip):
        return (area, here.layer_of(flip))

    loads = []
    thick_copy = pltpu.make_async_copy(thick, thick_s, thick_sem.at[0])
    thick_copy.start()
    for n, flip in enumerate(FLIPS):
        rows = here.rows(flip, 0, SLAB)
        group = [
            pltpu.make_async_copy(cap.at[rows], capv.at[rows], in_sem.at[n, 0]),
            pltpu.make_async_copy(plu.at[rows], pluv.at[rows], in_sem.at[n, 1]),
            pltpu.make_async_copy(perm.at[:, rows], permv.at[:, rows], in_sem.at[n, 2]),
            pltpu.make_async_copy(mob.at[:, rows], mobv.at[:, rows], in_sem.at[n, 3]),
        ]
        for copy in group:
            copy.start()
        loads.append(group)

    barrier = pltpu.get_barrier_semaphore()
    for flip in OTHERS:
        pl.semaphore_signal(barrier, inc=1, device_id=peer(flip), device_id_type=MESH)
    for step in (1, here.areas - 1):
        pl.semaphore_signal(
            barrier, inc=1, device_id=((area + step) % here.areas, layer), device_id_type=MESH
        )

    base = here.slab * SLAB
    sources = (cap, plu, sto, src, old)
    targets = (edge_i.at[0], edge_i.at[1], edge_f.at[0], edge_f.at[1], edge_f.at[2])

    def edge_copies(sem_row, first_row, count, at):
        rows = pl.ds(pl.multiple_of(base + first_row, 8), count)
        return [
            pltpu.make_async_copy(s.at[rows], t.at[pl.ds(at, count)], edge_sem.at[sem_row, n])
            for n, (s, t) in enumerate(zip(sources, targets))
        ]

    mid_copies = edge_copies(0, 0, SLAB, HALO)
    for copy in mid_copies:
        copy.start()

    @pl.when(here.slab > 0)
    def _():
        for copy in edge_copies(1, -HALO, HALO, 0):
            copy.start()

    @pl.when(here.slab < 7)
    def _():
        for copy in edge_copies(2, SLAB, HALO, HALO + SLAB):
            copy.start()

    thick_copy.wait()
    sublane = lax.broadcasted_iota(jnp.int32, (8, 128), 0)
    tile = jnp.zeros((8, 128), jnp.float32)
    for k in range(LAYERS):
        tile = jnp.where(sublane == k, thick_s[k], tile)
    thick_all[layer] = tile

    def input_sends():
        up = [
            pltpu.make_async_remote_copy(
                s.at[pl.ds(0, HALO)], t.at[pl.ds(HALO + SLAB, HALO)],
                input_send.at[0, n], input_recv.at[0, n],
                device_id=(area - 1, layer), device_id_type=MESH,
            )
            for n, (s, t) in enumerate(zip(sources, targets))
        ]
        down = [
            pltpu.make_async_remote_copy(
                s.at[pl.ds(ROWS - HALO, HALO)], t.at[pl.ds(0, HALO)],
                input_send.at[1, n], input_recv.at[1, n],
                device_id=(area + 1, layer), device_id_type=MESH,
            )
            for n, (s, t) in enumerate(zip(sources, targets))
        ]
        return up, down

    to_up, to_down = input_sends()
    crosses_up = is_first & (area > 0)
    crosses_down = is_last & (area < here.areas - 1)
    top_edge = is_first & (area == 0)
    bottom_edge = is_last & (area == here.areas - 1)

    def conduct_slab(n, flip):
        for copy in loads[n]:
            copy.wait()
        start = here.slab_of(flip) * SLAB

        @pl.loop(0, SLAB // 8)
        def _(i):
            rows = pl.ds(pl.multiple_of(start + i * 8, 8), 8)
            top = capv[rows, :]
            bottom = pluv[rows, :]
            trans = None
            for k in range(LAYERS):
                depth = layer * LAYERS + k
                flow = permv[k, rows, :] * mobv[k, rows, :] * thick_s[k]
                flow = jnp.where(depth >= top, flow, 0.0)
                cond[k, rows, :] = flow
                part = jnp.where(depth < bottom, flow, 0.0)
                trans, buoy = (flow, part) if trans is None else (trans + flow, buoy + part)
            tb[0, rows, :] = trans
            tb[1, rows, :] = buoy

    def rs_copy(q, number, rows, buffer, dim):
        return pltpu.make_async_remote_copy(
            tb.at[:, rows], buffer, rs_send.at[q, number], rs_recv.at[q, number],
            device_id=peer(flip_of(dim)), device_id_type=MESH,
        )

    PIECES = ((1, 1), (1, 0), (0, 1), (0, 0))

    def part_rows(q, flip):
        return here.rows(flip, PART_START[q], PART_ROWS[q])

    def first_copy(q, n):
        d1, d2, d3 = ORDERS[q]
        e2, e3 = PIECES[n]
        flip = flip_of(*([d1] + [d2] * e2 + [d3] * e3))
        return flip, rs_copy(q, n, part_rows(q, flip), r1[q].at[n], d1)

    def second_copy(q, n):
        d1, d2, d3 = ORDERS[q]
        flip = flip_of(*([d2] + ([d3] if n == 0 else [])))
        return flip, rs_copy(q, 4 + n, part_rows(q, flip), r2[q].at[n], d2)

    def third_copy(q):
        d1, d2, d3 = ORDERS[q]
        flip = flip_of(d3)
        return flip, rs_copy(q, 6, part_rows(q, flip), r3[q], d3)

    for n, flip in enumerate(FLIPS):
        conduct_slab(n, flip)
        if n == 0:
            pl.semaphore_wait(barrier, 9)
        for q in range(3):
            for m in range(4):
                owner, copy = first_copy(q, m)
                if owner == flip:
                    copy.start()
                    waits.append(copy)
        if n == 0:
            for m, other in enumerate(OTHERS):
                copy = pltpu.make_async_remote_copy(
                    thick_all.at[layer], thick_all.at[layer], th_send.at[m], th_recv.at[m],
                    device_id=peer(other), device_id_type=MESH,
                )
                copy.start()
                waits.append(copy)

            @pl.when(crosses_up)
            def _():
                for copy in to_up:
                    copy.start()

            @pl.when(crosses_down)
            def _():
                for copy in to_down:
                    copy.start()

    def row_copy(n, array):
        return pltpu.make_async_remote_copy(
            array.at[:, pl.ds(0, 8)], array.at[:, pl.ds(ROWS, 8)], row_send.at[n], row_recv.at[n],
            device_id=(area - 1, layer), device_id_type=MESH,
        )

    @pl.when(area > 0)
    def _():
        row_copy(0, cond).start()

    for m, other in enumerate(OTHERS):
        pltpu.make_async_remote_copy(
            thick_all.at[layer], thick_all.at[here.layer_of(other)], th_send.at[m], th_recv.at[m],
            device_id=peer(other), device_id_type=MESH,
        ).wait_recv()
    for block in range(8):
        for k in range(LAYERS):
            table[block * LAYERS + k] = jnp.broadcast_to(
                thick_all[block, pl.ds(k, 1), :], (8, 128)
            )

    def across(tile):
        return jnp.concatenate([tile] * (COLS // 128), axis=1)

    over_all = lax.fori_loop(
        0, layer * LAYERS, lambda z, total: total + table[z], jnp.zeros((8, 128), jnp.float32)
    )

    def gas_sum(blocks, top, bottom):
        def add_block(block, total):
            for k in range(LAYERS):
                depth = block * LAYERS + k
                inside = (depth >= top) & (depth < bottom)
                total = total + jnp.where(inside, across(table[depth]), 0.0)
            return total

        return lax.fori_loop(0, blocks, add_block, jnp.zeros(top.shape, jnp.float32))

    def heads(low, high):
        @pl.loop(low, high)
        def _(i):
            rows = pl.ds(pl.multiple_of(i * 8, 8), 8)
            top = capv[rows, :]
            bottom = pluv[rows, :]
            above = across(over_all) - (brine_density - gas_density) * gas_sum(layer, top, bottom)
            for k in range(LAYERS):
                depth = layer * LAYERS + k
                inside = (depth >= top) & (depth < bottom)
                mass = jnp.where(inside, gas_density * thick_s[k], brine_density * thick_s[k])
                hh[k, rows, :] = gravity_scale * (above + 0.5 * mass)
                above = above + mass

    lane_last = lax.broadcasted_iota(jnp.int32, (32, COLS), 1) < COLS - 1

    def faces(low, high):
        @pl.loop(low * LAYERS, high * LAYERS)
        def _(i):
            k = i % LAYERS
            start = pl.multiple_of((i // LAYERS) * 32, 8)
            flow = cond[k, pl.ds(start, 40), :]
            head = hh[k, pl.ds(start, 40), :]
            next_flow = pltpu.roll(flow, 39, 0)[:32]
            next_head = pltpu.roll(head, 39, 0)[:32]
            flow = flow[:32]
            head = head[:32]
            rows = pl.ds(start, 32)
            face = harmonic(flow, next_flow)
            hr[k, rows, :] = face
            gr[k, rows, :] = face * (head - next_head)
            side_flow = jnp.where(lane_last, pltpu.roll(flow, COLS - 1, 1), 0.0)
            side_head = pltpu.roll(head, COLS - 1, 1)
            face = harmonic(flow, side_flow)
            hc[k, rows, :] = face
            gc[k, rows, :] = face * (head - side_head)

    def second(n):
        for q in range(3):
            _, arrived = first_copy(q, n)
            arrived.wait_recv()
            flip, copy = second_copy(q, n)
            rows = part_rows(q, flip)
            tb[:, rows, :] = tb[:, rows, :] + r1[q][n]
            copy.start()
            waits.append(copy)

    second(0)
    heads(0, 32)
    second(1)
    heads(32, 64)

    @pl.when(area > 0)
    def _():
        row_copy(1, hh).start()

    for copy in mid_copies:
        copy.wait()

    @pl.when(here.slab > 0)
    def _():
        for copy in edge_copies(1, -HALO, HALO, 0):
            copy.wait()

    @pl.when(here.slab < 7)
    def _():
        for copy in edge_copies(2, SLAB, HALO, HALO + SLAB):
            copy.wait()

    @pl.when(crosses_up)
    def _():
        for copy in to_down:
            copy.wait_recv()

    @pl.when(crosses_down)
    def _():
        for copy in to_up:
            copy.wait_recv()

    def blank(at):
        rows = pl.ds(at, HALO)
        edge_i[:, rows, :] = jnp.zeros((2, HALO, COLS), jnp.int32)
        edge_f[0, rows, :] = jnp.ones((HALO, COLS), jnp.float32)
        edge_f[1, rows, :] = jnp.zeros((HALO, COLS), jnp.float32)
        edge_f[2, rows, :] = jnp.zeros((HALO, COLS), jnp.float32)
        wide[:, rows, :] = jnp.zeros((2, HALO, COLS), jnp.float32)

    @pl.when(top_edge)
    def _():
        blank(0)

    @pl.when(bottom_edge)
    def _():
        blank(HALO + SLAB)

    @pl.loop(0, WIDE // 8)
    def _(i):
        rows = pl.ds(pl.multiple_of(i * 8, 8), 8)
        gas[rows, :] = buoyancy_scale * gas_sum(8, edge_i[0, rows, :], edge_i[1, rows, :])

    faces(0, 5)

    for q in range(3):
        first_copy(q, 2)[1].wait_recv()
        second_copy(q, 0)[1].wait_recv()
        flip, copy = third_copy(q)
        rows = part_rows(q, flip)
        tb[:, rows, :] = tb[:, rows, :] + (r1[q][2] + r2[q][0])
        copy.start()
        waits.append(copy)

    faces(5, 15)

    @pl.when(area < here.areas - 1)
    def _():
        row_copy(0, cond).wait_recv()
        row_copy(1, hh).wait_recv()

    @pl.when(area == here.areas - 1)
    def _():
        cond[:, pl.ds(ROWS, 8), :] = jnp.zeros((LAYERS, 8, COLS), jnp.float32)
        hh[:, pl.ds(ROWS, 8), :] = jnp.zeros((LAYERS, 8, COLS), jnp.float32)

    faces(15, 16)

    for q in range(3):
        first_copy(q, 3)[1].wait_recv()
        second_copy(q, 1)[1].wait_recv()
        third_copy(q)[1].wait_recv()
        mine = part_rows(q, (0, 0, 0))
        at = pl.ds(HALO + PART_START[q], PART_ROWS[q])
        wide[:, at, :] = tb[:, mine, :] + r1[q][3] + (r2[q][1] + r3[q][...])

    up_area = area - (7 - here.slab) // 7
    up_same = 1 - (7 - here.slab) // 7
    down_area = area + here.slab // 7
    down_same = 1 - here.slab // 7
    up_layer = up_same * here.layer_of_slab(here.slab - up_same) + (1 - up_same) * layer
    down_layer = down_same * here.layer_of_slab(here.slab + down_same) + (1 - down_same) * layer
    halo_up = pltpu.make_async_remote_copy(
        wide.at[:, pl.ds(HALO, HALO)], wide.at[:, pl.ds(HALO + SLAB, HALO)],
        halo_send.at[0], halo_recv.at[0], device_id=(up_area, up_layer), device_id_type=MESH,
    )
    halo_down = pltpu.make_async_remote_copy(
        wide.at[:, pl.ds(SLAB, HALO)], wide.at[:, pl.ds(0, HALO)],
        halo_send.at[1], halo_recv.at[1], device_id=(down_area, down_layer), device_id_type=MESH,
    )
    has_up = area * 8 + here.slab > 0
    has_down = area * 8 + here.slab < here.areas * 8 - 1

    @pl.when(has_up)
    def _():
        halo_up.start()

    @pl.when(has_down)
    def _():
        halo_down.start()

    @pl.when(has_up)
    def _():
        halo_down.wait_recv()

    @pl.when(has_down)
    def _():
        halo_up.wait_recv()

    lane = lax.broadcasted_iota(jnp.int32, (WIDE, COLS), 1)

    def after(x):
        return pltpu.roll(x, WIDE - 1, 0)

    def before(x):
        return pltpu.roll(x, 1, 0)

    def right(x):
        return jnp.where(lane < COLS - 1, pltpu.roll(x, COLS - 1, 1), 0.0)

    def left(x):
        return jnp.where(lane > 0, pltpu.roll(x, 1, 1), 0.0)

    trans = wide[0]
    face_row = harmonic(trans, after(trans))
    t_row[...] = face_row
    face_col = harmonic(trans, right(trans))
    t_col[...] = face_col
    diagonal = edge_f[0] + face_row + before(face_row) + face_col + left(face_col)
    inverse[...] = 1.0 / diagonal
    buoy = wide[1]
    drive = gas[...]
    push = harmonic(buoy, after(buoy)) * (after(drive) - drive)
    total = push - before(push)
    push = harmonic(buoy, right(buoy)) * (right(drive) - drive)
    total = total + (push - left(push))
    right_hand[...] = edge_f[0] * edge_f[2] + edge_f[1] + total

    for sweep in range(SWEEPS):
        pressure = edge_f[2]
        face_row = t_row[...]
        face_col = t_col[...]
        inflow = face_row * after(pressure) + before(face_row * pressure)
        inflow = inflow + (face_col * right(pressure) + left(face_col * pressure))
        edge_f[2] = (right_hand[...] + inflow) * inverse[...]

    pf[here.rows((0, 0, 0), 0, SLAB), :] = edge_f[2, pl.ds(HALO, SLAB), :]

    @pl.when(is_last)
    def _():
        pf[pl.ds(ROWS, 8), :] = edge_f[2, pl.ds(HALO + SLAB, 8), :]

    def ag_copy(q, number, flip, dim):
        rows = part_rows(q, flip)
        return pltpu.make_async_remote_copy(
            pf.at[rows], pf.at[rows], ag_send.at[q, number], ag_recv.at[q, number],
            device_id=peer(flip_of(dim)), device_id_type=MESH,
        )

    def ag_arrival(q, number, flip, dim):
        merged = tuple((a + b) % 2 for a, b in zip(flip, flip_of(dim)))
        ag_copy(q, number, merged, dim).wait_recv()

    def ag_send_one(q, number, flip, dim):
        copy = ag_copy(q, number, flip, dim)
        copy.start()
        waits.append(copy)

    for which in (2, 1, 0):
        for q in range(3):
            ag_send_one(q, (0, 0, 0)[which] if which == 2 else (3, 1, 0)[which], (0, 0, 0), ORDERS[q][which])

    def last_copy(m, other):
        return pltpu.make_async_remote_copy(
            pf.at[pl.ds(ROWS, 8)], pf.at[pl.ds(ROWS, 8)], last_send.at[m], last_recv.at[0],
            device_id=peer(other), device_id_type=MESH,
        )

    @pl.when(is_last)
    def _():
        for m, other in enumerate(OTHERS):
            last_copy(m, other).start()

    for q in range(3):
        d1, d2, d3 = ORDERS[q]
        ag_arrival(q, 0, (0, 0, 0), d3)
        ag_send_one(q, 2, flip_of(d3), d2)
        ag_send_one(q, 4, flip_of(d3), d1)
    for q in range(3):
        d1, d2, d3 = ORDERS[q]
        ag_arrival(q, 1, (0, 0, 0), d2)
        ag_send_one(q, 5, flip_of(d2), d1)
    for q in range(3):
        d1, d2, d3 = ORDERS[q]
        ag_arrival(q, 2, flip_of(d3), d2)
        ag_send_one(q, 6, flip_of(d2, d3), d1)
    for number, dims in ((3, ()), (4, (2,)), (5, (1,)), (6, (1, 2))):
        for q in range(3):
            order = ORDERS[q]
            ag_arrival(q, number, flip_of(*[order[d] for d in dims]), order[0])

    @pl.when(here.slab < 7)
    def _():
        last_copy(0, OTHERS[0]).wait_recv()

    for copy in waits:
        copy.wait_send()

    @pl.when(is_last)
    def _():
        for m, other in enumerate(OTHERS):
            last_copy(m, other).wait_send()

    @pl.when(has_up)
    def _():
        halo_up.wait_send()

    @pl.when(has_down)
    def _():
        halo_down.wait_send()

    @pl.when(area > 0)
    def _():
        row_copy(0, cond).wait_send()
        row_copy(1, hh).wait_send()

    @pl.when(crosses_up)
    def _():
        for copy in to_up:
            copy.wait_send()

    @pl.when(crosses_down)
    def _():
        for copy in to_down:
            copy.wait_send()


CHUNK = 32


def write_kernel(hh, hr, gr, hc, gc, pf, cell, rows_out, cols_out, cell_v, rows_v, cols_v, sems):
    chunks = ROWS // CHUNK

    def copies(i):
        rows = pl.ds(pl.multiple_of(i * CHUNK, 8), CHUNK)
        return [
            pltpu.make_async_copy(v.at[:, rows], o.at[:, rows], sems.at[n, i])
            for n, (v, o) in enumerate(((cell_v, cell), (rows_v, rows_out), (cols_v, cols_out)))
        ]

    @pl.loop(0, chunks)
    def _(i):
        start = pl.multiple_of(i * CHUNK, 8)
        rows = pl.ds(start, CHUNK)
        wide = pf[pl.ds(start, CHUNK + 8), :]
        pressure = wide[:CHUNK]
        row_drop = pressure - pltpu.roll(wide, CHUNK + 7, 0)[:CHUNK]
        col_drop = pressure - pltpu.roll(pressure, COLS - 1, 1)
        for k in range(LAYERS):
            cell_v[k, rows, :] = pressure + hh[k, rows, :]
            rows_v[k, rows, :] = hr[k, rows, :] * row_drop + gr[k, rows, :]
            cols_v[k, rows, :] = hc[k, rows, :] * col_drop + gc[k, rows, :]
        for copy in copies(i):
            copy.start()

    @pl.loop(0, chunks)
    def _(i):
        for copy in copies(i):
            copy.wait()


def local(permeability, mobility, thickness, caprock, plume, storage, source, pressure_old):
    f32, i32 = jnp.float32, jnp.int32
    vmem = pl.BlockSpec(memory_space=pltpu.VMEM)
    hbm = pl.BlockSpec(memory_space=pltpu.HBM)
    dma = pltpu.SemaphoreType.DMA
    V = pltpu.VMEM
    full = V((LAYERS, ROWS, COLS), f32)
    tall = V((LAYERS, ROWS + 8, COLS), f32)
    arrays = (permeability, mobility, thickness, caprock, plume, storage, source, pressure_old)
    arrays = [pltpu.with_memory_space_constraint(x, pltpu.HBM) for x in arrays]
    kept = pl.pallas_call(
        gather_kernel,
        out_shape=[tall, full, full, full, full, V((ROWS + 8, COLS), f32)],
        in_specs=[hbm] * 8,
        out_specs=[vmem] * 6,
        scratch_shapes=[
            V((LAYERS, ROWS, COLS), f32), V((LAYERS, ROWS, COLS), f32), V((LAYERS, ROWS + 8, COLS), f32),
            V((ROWS, COLS), i32), V((ROWS, COLS), i32), V((2, ROWS, COLS), f32),
            *[V((4, 2, r, COLS), f32) for r in PART_ROWS],
            *[V((2, 2, r, COLS), f32) for r in PART_ROWS],
            *[V((2, r, COLS), f32) for r in PART_ROWS],
            V((2, WIDE, COLS), f32), V((2, WIDE, COLS), i32), V((3, WIDE, COLS), f32),
            pltpu.SMEM((LAYERS,), f32), V((8, 8, 128), f32), V((32, 8, 128), f32),
            *[V((WIDE, COLS), f32) for _ in range(5)],
            dma((8, 4)), dma((3, 5)), dma((1,)), dma((3, 7)), dma((3, 7)), dma((3, 7)), dma((3, 7)),
            dma((7,)), dma((7,)), dma((2,)), dma((2,)), dma((2, 5)), dma((2, 5)), dma((2,)), dma((2,)),
            dma((7,)), dma((1,)),
        ],
        compiler_params=pltpu.CompilerParams(
            collective_id=0, has_side_effects=True, vmem_limit_bytes=26 << 20
        ),
        name="gather",
    )(*arrays)
    return pl.pallas_call(
        write_kernel,
        out_shape=[jax.ShapeDtypeStruct((LAYERS, ROWS, COLS), f32)] * 3,
        in_specs=[vmem] * 6,
        out_specs=[hbm] * 3,
        scratch_shapes=[V((LAYERS, ROWS, COLS), f32)] * 3 + [dma((3, ROWS // CHUNK))],
        compiler_params=pltpu.CompilerParams(vmem_limit_bytes=16 << 20),
        name="write",
    )(*kept)


def solution(mesh):
    in_specs = (
        P("layer", "area", None),
        P("layer", "area", None),
        P("layer"),
        P("area", None),
        P("area", None),
        P("area", None),
        P("area", None),
        P("area", None),
    )
    out_specs = (P("layer", "area", None), P("layer", "area", None), P("layer", "area", None))
    return jax.shard_map(
        lambda *args: tuple(local(*args)), mesh=mesh, in_specs=in_specs, out_specs=out_specs, check_vma=False
    )
```

```python
import functools

import jax
import jax.numpy as jnp
from jax import lax
from jax.experimental import pallas as pl
from jax.experimental.pallas import tpu as pltpu
from jax.sharding import PartitionSpec as P

SWEEPS = 3
buoyancy_scale = 0.3
gravity_scale = 0.05
gas_density = 0.7
brine_density = 1.0

LAYERS = 4
ROWS = 512
COLS = 512
SLAB = 64
HALO = 8
WIDE = SLAB + 2 * HALO
MESH = pl.DeviceIdType.MESH

ORDERS = ((0, 1, 2), (1, 2, 0), (2, 0, 1))
PART_START = (0, 24, 48)
PART_ROWS = (24, 24, 16)
FLIPS = ((1, 1, 1), (1, 1, 0), (0, 1, 1), (1, 0, 1), (1, 0, 0), (0, 1, 0), (0, 0, 1), (0, 0, 0))
OTHERS = FLIPS[:-1]


def harmonic(near_value, far_value):
    summed = near_value + far_value
    divisor = jnp.where(summed > 0, summed, 1.0)
    return 2.0 * near_value * far_value / divisor


def flip_of(*dims):
    return tuple(1 if d in dims else 0 for d in range(3))


class Place:
    def __init__(self):
        self.area = lax.axis_index("area")
        self.layer = lax.axis_index("layer")
        self.areas = lax.axis_size("area")
        x = self.layer % 4
        second = x // 2
        first = (x % 2) + second - 2 * (x % 2) * second
        self.code = (first, second, self.layer // 4)
        self.parity = self.area % 2
        self.slab = self.slab_of((0, 0, 0))

    def flipped(self, flip):
        return tuple((1 - c) if f else c for c, f in zip(self.code, flip))

    def layer_of(self, flip):
        first, second, half = self.flipped(flip)
        x = 2 * second + first + second - 2 * first * second
        return half * 4 + x

    def slab_of(self, flip):
        first, second, half = self.flipped(flip)
        x = 2 * second + first + second - 2 * first * second
        order = x + half * (7 - 2 * x)
        return order + self.parity * (7 - 2 * order)

    def layer_of_slab(self, slab):
        order = slab + self.parity * (7 - 2 * slab)
        return order + (order // 4) * (11 - 2 * order)

    def rows(self, flip, start, count):
        return pl.ds(pl.multiple_of(self.slab_of(flip) * SLAB + start, 8), count)


def gather_kernel(
    perm, mob, thick, cap, plu, sto, src, old,
    hh, hr, gr, hc, gc, pf,
    permv, mobv, cond, capv, pluv, tb, r1a, r1b, r1c, r2a, r2b, r2c, r3a, r3b, r3c,
    edge_3d, edge_2d, tiles, parts, sums, cross,
    wide, edge_i, edge_f, thick_s, thick_all, table, gas, t_row, t_col, right_hand, inverse,
    in_sem, edge_sem, thick_sem, rs_send, rs_recv, ag_send, ag_recv, th_send, th_recv,
    part_load, part_send, part_recv, sum_send, sum_recv, ready,
    halo_send, halo_recv, input_send, input_recv, row_send, row_recv, last_send, last_recv,
):
    here = Place()
    area, layer = here.area, here.layer
    r1, r2, r3 = (r1a, r1b, r1c), (r2a, r2b, r2c), (r3a, r3b, r3c)
    waits = []
    is_first = here.slab == 0
    is_last = here.slab == 7

    def peer(flip):
        return (area, here.layer_of(flip))

    loads = []
    thick_copy = pltpu.make_async_copy(thick, thick_s, thick_sem.at[0])
    thick_copy.start()
    part_copies = []
    for side, first_row in ((0, 0), (1, ROWS - HALO)):
        rows = pl.ds(first_row, HALO)
        part_copies += [
            pltpu.make_async_copy(cap.at[rows], edge_2d.at[0, side], part_load.at[side, 0]),
            pltpu.make_async_copy(plu.at[rows], edge_2d.at[1, side], part_load.at[side, 1]),
            pltpu.make_async_copy(perm.at[:, rows], edge_3d.at[0, side], part_load.at[side, 2]),
            pltpu.make_async_copy(mob.at[:, rows], edge_3d.at[1, side], part_load.at[side, 3]),
        ]
    for copy in part_copies:
        copy.start()
    for n, flip in enumerate(FLIPS):
        rows = here.rows(flip, 0, SLAB)
        group = [
            pltpu.make_async_copy(cap.at[rows], capv.at[rows], in_sem.at[n, 0]),
            pltpu.make_async_copy(plu.at[rows], pluv.at[rows], in_sem.at[n, 1]),
            pltpu.make_async_copy(perm.at[:, rows], permv.at[:, rows], in_sem.at[n, 2]),
            pltpu.make_async_copy(mob.at[:, rows], mobv.at[:, rows], in_sem.at[n, 3]),
        ]
        for copy in group:
            copy.start()
        loads.append(group)

    barrier = pltpu.get_barrier_semaphore()
    for flip in OTHERS:
        pl.semaphore_signal(barrier, inc=1, device_id=peer(flip), device_id_type=MESH)
    both_sides = [((area + step) % here.areas, layer) for step in (1, here.areas - 1)]

    @pl.when(here.parity == 0)
    def _():
        for neighbour in both_sides:
            pl.semaphore_signal(barrier, inc=1, device_id=neighbour, device_id_type=MESH)

    base = here.slab * SLAB
    sources = (cap, plu, sto, src, old)
    targets = (edge_i.at[0], edge_i.at[1], edge_f.at[0], edge_f.at[1], edge_f.at[2])

    def edge_copies(sem_row, first_row, count, at):
        rows = pl.ds(pl.multiple_of(base + first_row, 8), count)
        return [
            pltpu.make_async_copy(s.at[rows], t.at[pl.ds(at, count)], edge_sem.at[sem_row, n])
            for n, (s, t) in enumerate(zip(sources, targets))
        ]

    mid_copies = edge_copies(0, 0, SLAB, HALO)
    for copy in mid_copies:
        copy.start()

    @pl.when(here.slab > 0)
    def _():
        for copy in edge_copies(1, -HALO, HALO, 0):
            copy.start()

    @pl.when(here.slab < 7)
    def _():
        for copy in edge_copies(2, SLAB, HALO, HALO + SLAB):
            copy.start()

    thick_copy.wait()
    sublane = lax.broadcasted_iota(jnp.int32, (8, 128), 0)
    tile = jnp.zeros((8, 128), jnp.float32)
    for k in range(LAYERS):
        tile = jnp.where(sublane == k, thick_s[k], tile)
    thick_all[layer] = tile

    def input_sends():
        up = [
            pltpu.make_async_remote_copy(
                s.at[pl.ds(0, HALO)], t.at[pl.ds(HALO + SLAB, HALO)],
                input_send.at[0, n], input_recv.at[0, n],
                device_id=(area - 1, layer), device_id_type=MESH,
            )
            for n, (s, t) in enumerate(zip(sources, targets))
        ]
        down = [
            pltpu.make_async_remote_copy(
                s.at[pl.ds(ROWS - HALO, HALO)], t.at[pl.ds(0, HALO)],
                input_send.at[1, n], input_recv.at[1, n],
                device_id=(area + 1, layer), device_id_type=MESH,
            )
            for n, (s, t) in enumerate(zip(sources, targets))
        ]
        return up, down

    to_up, to_down = input_sends()
    crosses_up = is_first & (area > 0)
    crosses_down = is_last & (area < here.areas - 1)
    top_edge = is_first & (area == 0)
    bottom_edge = is_last & (area == here.areas - 1)

    sub8 = lax.broadcasted_iota(jnp.int32, (8, COLS), 0)
    for copy in part_copies:
        copy.wait()
    for side in (0, 1):
        top = edge_2d[0, side]
        bottom = edge_2d[1, side]
        trans = buoy = jnp.zeros((8, COLS), jnp.float32)
        for k in range(LAYERS):
            depth = layer * LAYERS + k
            flow = edge_3d[0, side, k] * edge_3d[1, side, k] * thick_s[k]
            flow = jnp.where(depth >= top, flow, 0.0)
            trans = trans + flow
            buoy = buoy + jnp.where(depth < bottom, flow, 0.0)
        used = (sub8 < 4) if side == 0 else (sub8 >= 4)
        tiles[side] = jnp.where(used, trans, pltpu.roll(buoy, 4, 0))

    pl.semaphore_wait(barrier, 7 + 2 * here.parity)

    @pl.when(here.parity == 1)
    def _():
        for neighbour in both_sides:
            pl.semaphore_signal(ready, inc=1, device_id=neighbour, device_id_type=MESH)

    def part_copy(m, side):
        return pltpu.make_async_remote_copy(
            tiles.at[side], parts.at[m], part_send.at[side], part_recv.at[m],
            device_id=peer(OTHERS[m]), device_id_type=MESH,
        )

    for m, other in enumerate(OTHERS):
        for side, owner in ((0, 0), (1, 7)):

            @pl.when(here.slab_of(other) == owner)
            def _(m=m, side=side):
                part_copy(m, side).start()

    for m, other in enumerate(OTHERS):
        copy = pltpu.make_async_remote_copy(
            thick_all.at[layer], thick_all.at[layer], th_send.at[m], th_recv.at[m],
            device_id=peer(other), device_id_type=MESH,
        )
        copy.start()
        waits.append(copy)

    def conduct_slab(n, flip):
        for copy in loads[n]:
            copy.wait()
        start = here.slab_of(flip) * SLAB

        @pl.loop(0, SLAB // 8)
        def _(i):
            rows = pl.ds(pl.multiple_of(start + i * 8, 8), 8)
            top = capv[rows, :]
            bottom = pluv[rows, :]
            trans = None
            for k in range(LAYERS):
                depth = layer * LAYERS + k
                flow = permv[k, rows, :] * mobv[k, rows, :] * thick_s[k]
                flow = jnp.where(depth >= top, flow, 0.0)
                cond[k, rows, :] = flow
                part = jnp.where(depth < bottom, flow, 0.0)
                trans, buoy = (flow, part) if trans is None else (trans + flow, buoy + part)
            tb[0, rows, :] = trans
            tb[1, rows, :] = buoy

    def rs_copy(q, number, rows, buffer, dim):
        return pltpu.make_async_remote_copy(
            tb.at[:, rows], buffer, rs_send.at[q, number], rs_recv.at[q, number],
            device_id=peer(flip_of(dim)), device_id_type=MESH,
        )

    PIECES = ((1, 1), (1, 0), (0, 1), (0, 0))

    def part_rows(q, flip):
        return here.rows(flip, PART_START[q], PART_ROWS[q])

    def first_copy(q, n):
        d1, d2, d3 = ORDERS[q]
        e2, e3 = PIECES[n]
        flip = flip_of(*([d1] + [d2] * e2 + [d3] * e3))
        return flip, rs_copy(q, n, part_rows(q, flip), r1[q].at[n], d1)

    def second_copy(q, n):
        d1, d2, d3 = ORDERS[q]
        flip = flip_of(*([d2] + ([d3] if n == 0 else [])))
        return flip, rs_copy(q, 4 + n, part_rows(q, flip), r2[q].at[n], d2)

    def third_copy(q):
        d1, d2, d3 = ORDERS[q]
        flip = flip_of(d3)
        return flip, rs_copy(q, 6, part_rows(q, flip), r3[q], d3)

    for n, flip in enumerate(FLIPS):
        conduct_slab(n, flip)
        for q in range(3):
            for m in range(4):
                owner, copy = first_copy(q, m)
                if owner == flip:
                    copy.start()
                    waits.append(copy)

    def row_copy(n, array):
        return pltpu.make_async_remote_copy(
            array.at[:, pl.ds(0, 8)], array.at[:, pl.ds(ROWS, 8)], row_send.at[n], row_recv.at[n],
            device_id=(area - 1, layer), device_id_type=MESH,
        )

    def across(tile):
        return jnp.concatenate([tile] * (COLS // 128), axis=1)

    def gas_sum(blocks, top, bottom):
        def lookup(index, count):
            def step(block, found):
                for k in range(LAYERS):
                    depth = block * LAYERS + k
                    found = jnp.where(depth < index, across(table[depth + 1]), found)
                return found

            return lax.fori_loop(0, count, step, jnp.zeros(index.shape, jnp.float32))

        return jnp.maximum(lookup(bottom, blocks) - lookup(top, jnp.minimum(blocks, 4)), 0.0)

    def heads(low, high):
        @pl.loop(low, high)
        def _(i):
            rows = pl.ds(pl.multiple_of(i * 8, 8), 8)
            top = capv[rows, :]
            bottom = pluv[rows, :]
            above = across(table[layer * LAYERS]) - (brine_density - gas_density) * gas_sum(layer, top, bottom)
            for k in range(LAYERS):
                depth = layer * LAYERS + k
                inside = (depth >= top) & (depth < bottom)
                mass = jnp.where(inside, gas_density * thick_s[k], brine_density * thick_s[k])
                hh[k, rows, :] = gravity_scale * (above + 0.5 * mass)
                above = above + mass

    lane_last = lax.broadcasted_iota(jnp.int32, (32, COLS), 1) < COLS - 1

    def faces(low, high):
        @pl.loop(low * LAYERS, high * LAYERS)
        def _(i):
            k = i % LAYERS
            start = pl.multiple_of((i // LAYERS) * 32, 8)
            flow = cond[k, pl.ds(start, 40), :]
            head = hh[k, pl.ds(start, 40), :]
            next_flow = pltpu.roll(flow, 39, 0)[:32]
            next_head = pltpu.roll(head, 39, 0)[:32]
            flow = flow[:32]
            head = head[:32]
            rows = pl.ds(start, 32)
            face = harmonic(flow, next_flow)
            hr[k, rows, :] = face
            gr[k, rows, :] = face * (head - next_head)
            side_flow = jnp.where(lane_last, pltpu.roll(flow, COLS - 1, 1), 0.0)
            side_head = pltpu.roll(head, COLS - 1, 1)
            face = harmonic(flow, side_flow)
            hc[k, rows, :] = face
            gc[k, rows, :] = face * (head - side_head)

    def second(n):
        for q in range(3):
            _, arrived = first_copy(q, n)
            arrived.wait_recv()
            flip, copy = second_copy(q, n)
            rows = part_rows(q, flip)
            tb[:, rows, :] = tb[:, rows, :] + r1[q][n]
            copy.start()
            waits.append(copy)

    forward_up = pltpu.make_async_remote_copy(
        sums, cross.at[1], sum_send.at[0], sum_recv.at[1],
        device_id=(area - 1, layer), device_id_type=MESH,
    )
    forward_down = pltpu.make_async_remote_copy(
        sums, cross.at[0], sum_send.at[0], sum_recv.at[0],
        device_id=(area + 1, layer), device_id_type=MESH,
    )

    def forward_edges():
        for ends, side in ((is_first, 0), (is_last, 1)):

            @pl.when(ends)
            def _(side=side):
                for m in range(7):
                    part_copy(m, side).wait_recv()
                total = tiles[side]
                for m in range(7):
                    total = total + parts[m]
                sums[...] = total

        @pl.when(crosses_up)
        def _():
            for copy in (forward_up, *to_up):
                copy.start()

        @pl.when(crosses_down)
        def _():
            for copy in (forward_down, *to_down):
                copy.start()

        @pl.when(area > 0)
        def _():
            row_copy(0, cond).start()

    def gas_rows(at):
        rows = pl.ds(at, 8)
        gas[rows, :] = buoyancy_scale * gas_sum(8, edge_i[0, rows, :], edge_i[1, rows, :])

    @pl.when(here.parity == 1)
    def _():
        forward_edges()

    second(0)

    for m, other in enumerate(OTHERS):
        pltpu.make_async_remote_copy(
            thick_all.at[layer], thick_all.at[here.layer_of(other)], th_send.at[m], th_recv.at[m],
            device_id=peer(other), device_id_type=MESH,
        ).wait_recv()
    total = jnp.zeros((8, 128), jnp.float32)
    table[0] = total
    for block in range(8):
        for k in range(LAYERS):
            total = total + jnp.broadcast_to(thick_all[block, pl.ds(k, 1), :], (8, 128))
            table[block * LAYERS + k + 1] = total


    second(1)
    heads(0, 32)

    @pl.when(here.parity == 0)
    def _():
        pl.semaphore_wait(ready, 2)
        forward_edges()

    for copy in mid_copies:
        copy.wait()

    @pl.when(here.slab > 0)
    def _():
        for copy in edge_copies(1, -HALO, HALO, 0):
            copy.wait()

    @pl.when(here.slab < 7)
    def _():
        for copy in edge_copies(2, SLAB, HALO, HALO + SLAB):
            copy.wait()

    for q in range(3):
        first_copy(q, 2)[1].wait_recv()
        second_copy(q, 0)[1].wait_recv()
        flip, copy = third_copy(q)
        rows = part_rows(q, flip)
        tb[:, rows, :] = tb[:, rows, :] + (r1[q][2] + r2[q][0])
        copy.start()
        waits.append(copy)

    heads(32, 64)

    @pl.when(area > 0)
    def _():
        row_copy(1, hh).start()

    @pl.loop(1, WIDE // 8 - 1)
    def _(i):
        gas_rows(pl.multiple_of(i * 8, 8))

    for q in range(3):
        first_copy(q, 3)[1].wait_recv()
        second_copy(q, 1)[1].wait_recv()
        third_copy(q)[1].wait_recv()
        mine = part_rows(q, (0, 0, 0))
        at = pl.ds(HALO + PART_START[q], PART_ROWS[q])
        wide[:, at, :] = tb[:, mine, :] + r1[q][3] + (r2[q][1] + r3[q][...])

    up_layer = here.layer_of_slab(jnp.maximum(here.slab - 1, 0))
    down_layer = here.layer_of_slab(jnp.minimum(here.slab + 1, 7))
    halo_up = pltpu.make_async_remote_copy(
        wide.at[:, pl.ds(HALO, HALO)], wide.at[:, pl.ds(HALO + SLAB, HALO)],
        halo_send.at[0], halo_recv.at[0], device_id=(area, up_layer), device_id_type=MESH,
    )
    halo_down = pltpu.make_async_remote_copy(
        wide.at[:, pl.ds(SLAB, HALO)], wide.at[:, pl.ds(0, HALO)],
        halo_send.at[1], halo_recv.at[1], device_id=(area, down_layer), device_id_type=MESH,
    )

    @pl.when(here.slab > 0)
    def _():
        halo_up.start()

    @pl.when(here.slab < 7)
    def _():
        halo_down.start()

    def blank(at):
        rows = pl.ds(at, HALO)
        edge_i[:, rows, :] = jnp.zeros((2, HALO, COLS), jnp.int32)
        edge_f[0, rows, :] = jnp.ones((HALO, COLS), jnp.float32)
        edge_f[1, rows, :] = jnp.zeros((HALO, COLS), jnp.float32)
        edge_f[2, rows, :] = jnp.zeros((HALO, COLS), jnp.float32)
        wide[:, rows, :] = jnp.zeros((2, HALO, COLS), jnp.float32)

    def unpack(slot, at, used):
        rows = pl.ds(at, HALO)
        tile = cross[slot]
        wide[0, rows, :] = jnp.where(used, tile, 0.0)
        wide[1, rows, :] = jnp.where(used, pltpu.roll(tile, 4, 0), 0.0)

    @pl.when(top_edge)
    def _():
        blank(0)

    @pl.when(bottom_edge)
    def _():
        blank(HALO + SLAB)

    @pl.when(crosses_up)
    def _():
        for copy in (forward_down, *to_down):
            copy.wait_recv()
        unpack(0, 0, sub8 >= 4)

    @pl.when(crosses_down)
    def _():
        for copy in (forward_up, *to_up):
            copy.wait_recv()
        unpack(1, HALO + SLAB, sub8 < 4)

    gas_rows(0)
    gas_rows(HALO + SLAB)

    @pl.when(here.slab > 0)
    def _():
        halo_down.wait_recv()

    @pl.when(here.slab < 7)
    def _():
        halo_up.wait_recv()

    lane = lax.broadcasted_iota(jnp.int32, (WIDE, COLS), 1)

    def after(x):
        return pltpu.roll(x, WIDE - 1, 0)

    def before(x):
        return pltpu.roll(x, 1, 0)

    def right(x):
        return jnp.where(lane < COLS - 1, pltpu.roll(x, COLS - 1, 1), 0.0)

    def left(x):
        return jnp.where(lane > 0, pltpu.roll(x, 1, 1), 0.0)

    trans = wide[0]
    face_row = harmonic(trans, after(trans))
    t_row[...] = face_row
    face_col = harmonic(trans, right(trans))
    t_col[...] = face_col
    diagonal = edge_f[0] + face_row + before(face_row) + face_col + left(face_col)
    inverse[...] = 1.0 / diagonal
    buoy = wide[1]
    drive = gas[...]
    push = harmonic(buoy, after(buoy)) * (after(drive) - drive)
    total = push - before(push)
    push = harmonic(buoy, right(buoy)) * (right(drive) - drive)
    total = total + (push - left(push))
    right_hand[...] = edge_f[0] * edge_f[2] + edge_f[1] + total

    for sweep in range(SWEEPS):
        pressure = edge_f[2]
        face_row = t_row[...]
        face_col = t_col[...]
        inflow = face_row * after(pressure) + before(face_row * pressure)
        inflow = inflow + (face_col * right(pressure) + left(face_col * pressure))
        edge_f[2] = (right_hand[...] + inflow) * inverse[...]

    pf[here.rows((0, 0, 0), 0, SLAB), :] = edge_f[2, pl.ds(HALO, SLAB), :]

    @pl.when(is_last)
    def _():
        pf[pl.ds(ROWS, 8), :] = edge_f[2, pl.ds(HALO + SLAB, 8), :]

    def ag_copy(q, number, flip, dim):
        rows = part_rows(q, flip)
        return pltpu.make_async_remote_copy(
            pf.at[rows], pf.at[rows], ag_send.at[q, number], ag_recv.at[q, number],
            device_id=peer(flip_of(dim)), device_id_type=MESH,
        )

    def ag_arrival(q, number, flip, dim):
        merged = tuple((a + b) % 2 for a, b in zip(flip, flip_of(dim)))
        ag_copy(q, number, merged, dim).wait_recv()

    def ag_send_one(q, number, flip, dim):
        copy = ag_copy(q, number, flip, dim)
        copy.start()
        waits.append(copy)

    for which in (2, 1, 0):
        for q in range(3):
            ag_send_one(q, (0, 0, 0)[which] if which == 2 else (3, 1, 0)[which], (0, 0, 0), ORDERS[q][which])

    def last_copy(m, other):
        return pltpu.make_async_remote_copy(
            pf.at[pl.ds(ROWS, 8)], pf.at[pl.ds(ROWS, 8)], last_send.at[m], last_recv.at[0],
            device_id=peer(other), device_id_type=MESH,
        )

    @pl.when(is_last)
    def _():
        for m, other in enumerate(OTHERS):
            last_copy(m, other).start()

    faces(0, 4)
    for q in range(3):
        d1, d2, d3 = ORDERS[q]
        ag_arrival(q, 0, (0, 0, 0), d3)
        ag_send_one(q, 2, flip_of(d3), d2)
        ag_send_one(q, 4, flip_of(d3), d1)
    faces(4, 8)
    for q in range(3):
        d1, d2, d3 = ORDERS[q]
        ag_arrival(q, 1, (0, 0, 0), d2)
        ag_send_one(q, 5, flip_of(d2), d1)
    faces(8, 11)
    for q in range(3):
        d1, d2, d3 = ORDERS[q]
        ag_arrival(q, 2, flip_of(d3), d2)
        ag_send_one(q, 6, flip_of(d2, d3), d1)
    faces(11, 15)

    @pl.when(area < here.areas - 1)
    def _():
        row_copy(0, cond).wait_recv()
        row_copy(1, hh).wait_recv()

    @pl.when(area == here.areas - 1)
    def _():
        cond[:, pl.ds(ROWS, 8), :] = jnp.zeros((LAYERS, 8, COLS), jnp.float32)
        hh[:, pl.ds(ROWS, 8), :] = jnp.zeros((LAYERS, 8, COLS), jnp.float32)

    faces(15, 16)
    for number, dims in ((3, ()), (4, (2,)), (5, (1,)), (6, (1, 2))):
        for q in range(3):
            order = ORDERS[q]
            ag_arrival(q, number, flip_of(*[order[d] for d in dims]), order[0])

    @pl.when(here.slab < 7)
    def _():
        last_copy(0, OTHERS[0]).wait_recv()

    for copy in waits:
        copy.wait_send()

    @pl.when(is_last)
    def _():
        for m, other in enumerate(OTHERS):
            last_copy(m, other).wait_send()

    @pl.when(here.slab > 0)
    def _():
        halo_up.wait_send()

    @pl.when(here.slab < 7)
    def _():
        halo_down.wait_send()

    @pl.when(is_first == False)
    def _():
        part_copy(0, 0).wait_send()

    @pl.when(is_last == False)
    def _():
        part_copy(0, 1).wait_send()

    @pl.when(area > 0)
    def _():
        row_copy(0, cond).wait_send()
        row_copy(1, hh).wait_send()

    @pl.when(crosses_up)
    def _():
        for copy in (forward_up, *to_up):
            copy.wait_send()

    @pl.when(crosses_down)
    def _():
        for copy in (forward_down, *to_down):
            copy.wait_send()


CHUNK = 32


def write_kernel(hh, hr, gr, hc, gc, pf, cell, rows_out, cols_out, cell_v, rows_v, cols_v, sems):
    chunks = ROWS // CHUNK

    def copies(i):
        rows = pl.ds(pl.multiple_of(i * CHUNK, 8), CHUNK)
        return [
            pltpu.make_async_copy(v.at[:, rows], o.at[:, rows], sems.at[n, i])
            for n, (v, o) in enumerate(((cell_v, cell), (rows_v, rows_out), (cols_v, cols_out)))
        ]

    @pl.loop(0, chunks)
    def _(i):
        start = pl.multiple_of(i * CHUNK, 8)
        rows = pl.ds(start, CHUNK)
        wide = pf[pl.ds(start, CHUNK + 8), :]
        pressure = wide[:CHUNK]
        row_drop = pressure - pltpu.roll(wide, CHUNK + 7, 0)[:CHUNK]
        col_drop = pressure - pltpu.roll(pressure, COLS - 1, 1)
        for k in range(LAYERS):
            cell_v[k, rows, :] = pressure + hh[k, rows, :]
            rows_v[k, rows, :] = hr[k, rows, :] * row_drop + gr[k, rows, :]
            cols_v[k, rows, :] = hc[k, rows, :] * col_drop + gc[k, rows, :]
        for copy in copies(i):
            copy.start()

    @pl.loop(0, chunks)
    def _(i):
        for copy in copies(i):
            copy.wait()


def local(permeability, mobility, thickness, caprock, plume, storage, source, pressure_old):
    f32, i32 = jnp.float32, jnp.int32
    vmem = pl.BlockSpec(memory_space=pltpu.VMEM)
    hbm = pl.BlockSpec(memory_space=pltpu.HBM)
    dma = pltpu.SemaphoreType.DMA
    V = pltpu.VMEM
    full = V((LAYERS, ROWS, COLS), f32)
    tall = V((LAYERS, ROWS + 8, COLS), f32)
    arrays = (permeability, mobility, thickness, caprock, plume, storage, source, pressure_old)
    arrays = [pltpu.with_memory_space_constraint(x, pltpu.HBM) for x in arrays]
    kept = pl.pallas_call(
        gather_kernel,
        out_shape=[tall, full, full, full, full, V((ROWS + 8, COLS), f32)],
        in_specs=[hbm] * 8,
        out_specs=[vmem] * 6,
        scratch_shapes=[
            V((LAYERS, ROWS, COLS), f32), V((LAYERS, ROWS, COLS), f32), V((LAYERS, ROWS + 8, COLS), f32),
            V((ROWS, COLS), i32), V((ROWS, COLS), i32), V((2, ROWS, COLS), f32),
            *[V((4, 2, r, COLS), f32) for r in PART_ROWS],
            *[V((2, 2, r, COLS), f32) for r in PART_ROWS],
            *[V((2, r, COLS), f32) for r in PART_ROWS],
            V((2, 2, LAYERS, 8, COLS), f32), V((2, 2, 8, COLS), i32), V((2, 8, COLS), f32),
            V((7, 8, COLS), f32), V((8, COLS), f32), V((2, 8, COLS), f32),
            V((2, WIDE, COLS), f32), V((2, WIDE, COLS), i32), V((3, WIDE, COLS), f32),
            pltpu.SMEM((LAYERS,), f32), V((8, 8, 128), f32), V((33, 8, 128), f32),
            *[V((WIDE, COLS), f32) for _ in range(5)],
            dma((8, 4)), dma((3, 5)), dma((1,)), dma((3, 7)), dma((3, 7)), dma((3, 7)), dma((3, 7)),
            dma((7,)), dma((7,)),
            dma((2, 4)), dma((2,)), dma((7,)), dma((1,)), dma((2,)), pltpu.SemaphoreType.REGULAR,
            dma((2,)), dma((2,)), dma((2, 5)), dma((2, 5)), dma((2,)), dma((2,)),
            dma((7,)), dma((1,)),
        ],
        compiler_params=pltpu.CompilerParams(
            collective_id=0, has_side_effects=True, vmem_limit_bytes=26 << 20
        ),
        name="gather",
    )(*arrays)
    return pl.pallas_call(
        write_kernel,
        out_shape=[jax.ShapeDtypeStruct((LAYERS, ROWS, COLS), f32)] * 3,
        in_specs=[vmem] * 6,
        out_specs=[hbm] * 3,
        scratch_shapes=[V((LAYERS, ROWS, COLS), f32)] * 3 + [dma((3, ROWS // CHUNK))],
        compiler_params=pltpu.CompilerParams(vmem_limit_bytes=16 << 20),
        name="write",
    )(*kept)


def solution(mesh):
    in_specs = (
        P("layer", "area", None),
        P("layer", "area", None),
        P("layer"),
        P("area", None),
        P("area", None),
        P("area", None),
        P("area", None),
        P("area", None),
    )
    out_specs = (P("layer", "area", None), P("layer", "area", None), P("layer", "area", None))
    return jax.shard_map(
        lambda *args: tuple(local(*args)), mesh=mesh, in_specs=in_specs, out_specs=out_specs, check_vma=False
    )
```

```python
import functools

import jax
import jax.numpy as jnp
from jax import lax
from jax.experimental import pallas as pl
from jax.experimental.pallas import tpu as pltpu
from jax.sharding import PartitionSpec as P

SWEEPS = 3
buoyancy_scale = 0.3
gravity_scale = 0.05
gas_density = 0.7
brine_density = 1.0

LAYERS = 4
ROWS = 512
COLS = 512
HALVES = 2
HALF_ROWS = ROWS // HALVES
SLAB = 32
HALO = 8
WIDE = SLAB + 2 * HALO
MESH = pl.DeviceIdType.MESH

ORDERS = ((0, 1, 2), (1, 2, 0), (2, 0, 1))
PART_START = ((0, 16, 24), (0, 8, 24))
PART_ROWS = ((16, 8, 8), (8, 16, 8))
X_FIRST = (16, 8)
ACROSS = ((1, 1, 0), (1, 0, 0), (0, 1, 0))
OTHER_HALF = (0, 0, 1)
OWN = (0, 0, 0)
FLIPS = ((1, 1, 1), (1, 1, 0), (0, 1, 1), (1, 0, 1), (1, 0, 0), (0, 1, 0), (0, 0, 1), (0, 0, 0))
OTHERS = FLIPS[:-1]


def harmonic(near_value, far_value):
    summed = near_value + far_value
    divisor = jnp.where(summed > 0, summed, 1.0)
    return 2.0 * near_value * far_value / divisor


def flip_of(*dims):
    return tuple(1 if d in dims else 0 for d in range(3))


def plus(one, two):
    return tuple((a + b) % 2 for a, b in zip(one, two))


class Place:
    def __init__(self):
        self.area = lax.axis_index("area")
        self.layer = lax.axis_index("layer")
        self.areas = lax.axis_size("area")
        x = self.layer % 4
        second = x // 2
        first = (x % 2) + second - 2 * (x % 2) * second
        self.code = (first, second, self.layer // 4)
        self.parity = self.area % 2
        self.order = self.order_of(OWN)

    def flipped(self, flip):
        return tuple((1 - c) if f else c for c, f in zip(self.code, flip))

    def layer_of(self, flip):
        first, second, half = self.flipped(flip)
        x = 2 * second + first + second - 2 * first * second
        return half * 4 + x

    def order_of(self, flip):
        first, second, half = self.flipped(flip)
        x = 2 * second + first + second - 2 * first * second
        return x + half * (7 - 2 * x)

    def layer_at(self, order):
        return order + (order // 4) * (11 - 2 * order)

    def base(self, h, flip):
        order = self.order_of(flip)
        return h * HALF_ROWS + (7 - order if h else order) * SLAB

    def rows(self, h, flip, start, count):
        return pl.ds(pl.multiple_of(self.base(h, flip) + start, 8), count)


def gather_kernel(*refs):
    perm, mob, thick, cap, plu, sto, src, old = refs[:8]
    hh, hr, gr, hc, gc, pf = refs[8:14]
    r1 = [refs[14 + 3 * h : 17 + 3 * h] for h in range(HALVES)]
    r2 = [refs[20 + 3 * h : 23 + 3 * h] for h in range(HALVES)]
    r3 = [refs[26 + 3 * h : 29 + 3 * h] for h in range(HALVES)]
    (
        permv, mobv, cond, capv, pluv, tb,
        edge_3d, edge_2d, tiles, parts, sums, cross,
        wide, edge_i, edge_f, thick_s, thick_all, table, gas, t_row, t_col, right_hand, inverse,
        in_sem, edge_sem, thick_sem, rs_send, rs_recv, ag_send, ag_recv, th_send, th_recv,
        part_load, part_send, part_recv, sum_send, sum_recv, ready,
        halo_send, halo_recv, input_send, input_recv, row_send, row_recv, last_send, last_recv,
    ) = refs[32:]
    here = Place()
    area, layer = here.area, here.layer
    waits = []
    at_ends = here.order == 0
    at_middle = here.order == 7

    def peer(flip):
        return (area, here.layer_of(flip))

    loads = []
    thick_copy = pltpu.make_async_copy(thick, thick_s, thick_sem.at[0])
    thick_copy.start()
    part_copies = []
    for side, first_row in enumerate((0, ROWS - HALO, HALF_ROWS, HALF_ROWS - HALO)):
        rows = pl.ds(first_row, HALO)
        part_copies += [
            pltpu.make_async_copy(cap.at[rows], edge_2d.at[0, side], part_load.at[side, 0]),
            pltpu.make_async_copy(plu.at[rows], edge_2d.at[1, side], part_load.at[side, 1]),
            pltpu.make_async_copy(perm.at[:, rows], edge_3d.at[0, side], part_load.at[side, 2]),
            pltpu.make_async_copy(mob.at[:, rows], edge_3d.at[1, side], part_load.at[side, 3]),
        ]
    for copy in part_copies:
        copy.start()
    blocks = [(h, flip) for h in range(HALVES) for flip in FLIPS]
    for n, (h, flip) in enumerate(blocks):
        rows = here.rows(h, flip, 0, SLAB)
        group = [
            pltpu.make_async_copy(cap.at[rows], capv.at[rows], in_sem.at[n, 0]),
            pltpu.make_async_copy(plu.at[rows], pluv.at[rows], in_sem.at[n, 1]),
            pltpu.make_async_copy(perm.at[:, rows], permv.at[:, rows], in_sem.at[n, 2]),
            pltpu.make_async_copy(mob.at[:, rows], mobv.at[:, rows], in_sem.at[n, 3]),
        ]
        for copy in group:
            copy.start()
        loads.append(group)

    barrier = pltpu.get_barrier_semaphore()
    for flip in OTHERS:
        pl.semaphore_signal(barrier, inc=1, device_id=peer(flip), device_id_type=MESH)
    both_sides = [((area + step) % here.areas, layer) for step in (1, here.areas - 1)]

    @pl.when(here.parity == 0)
    def _():
        for neighbour in both_sides:
            pl.semaphore_signal(barrier, inc=1, device_id=neighbour, device_id_type=MESH)

    sources = (cap, plu, sto, src, old)

    def edge_targets(h):
        return (edge_i.at[h, 0], edge_i.at[h, 1], edge_f.at[h, 0], edge_f.at[h, 1], edge_f.at[h, 2])

    def edge_copies(sem_row, h, at, count):
        rows = here.rows(h, OWN, at - HALO, count)
        return [
            pltpu.make_async_copy(s.at[rows], t.at[pl.ds(at, count)], edge_sem.at[sem_row, n])
            for n, (s, t) in enumerate(zip(sources, edge_targets(h)))
        ]

    always = [edge_copies(0, 0, HALO, SLAB + HALO), edge_copies(1, 1, 0, SLAB + HALO)]

    def sometimes(h):
        return edge_copies(2 + h, h, h * (HALO + SLAB), HALO)

    for copy in (*always[0], *always[1]):
        copy.start()

    @pl.when(here.order > 0)
    def _():
        for h in range(HALVES):
            for copy in sometimes(h):
                copy.start()

    thick_copy.wait()
    sublane = lax.broadcasted_iota(jnp.int32, (8, 128), 0)
    tile = jnp.zeros((8, 128), jnp.float32)
    for k in range(LAYERS):
        tile = jnp.where(sublane == k, thick_s[k], tile)
    thick_all[layer] = tile

    def input_sends():
        up = [
            pltpu.make_async_remote_copy(
                s.at[pl.ds(0, HALO)], t.at[pl.ds(HALO + SLAB, HALO)],
                input_send.at[0, n], input_recv.at[0, n],
                device_id=(area - 1, layer), device_id_type=MESH,
            )
            for n, (s, t) in enumerate(zip(sources, edge_targets(1)))
        ]
        down = [
            pltpu.make_async_remote_copy(
                s.at[pl.ds(ROWS - HALO, HALO)], t.at[pl.ds(0, HALO)],
                input_send.at[1, n], input_recv.at[1, n],
                device_id=(area + 1, layer), device_id_type=MESH,
            )
            for n, (s, t) in enumerate(zip(sources, edge_targets(0)))
        ]
        return up, down

    to_up, to_down = input_sends()
    crosses_up = at_ends & (area > 0)
    crosses_down = at_ends & (area < here.areas - 1)
    top_edge = at_ends & (area == 0)
    bottom_edge = at_ends & (area == here.areas - 1)

    sub8 = lax.broadcasted_iota(jnp.int32, (8, COLS), 0)
    for copy in part_copies:
        copy.wait()
    for side in range(4):
        top = edge_2d[0, side]
        bottom = edge_2d[1, side]
        trans = buoy = jnp.zeros((8, COLS), jnp.float32)
        for k in range(LAYERS):
            depth = layer * LAYERS + k
            flow = edge_3d[0, side, k] * edge_3d[1, side, k] * thick_s[k]
            flow = jnp.where(depth >= top, flow, 0.0)
            trans = trans + flow
            buoy = buoy + jnp.where(depth < bottom, flow, 0.0)
        used = (sub8 < 4) if side % 2 == 0 else (sub8 >= 4)
        tiles[side // 2, side % 2] = jnp.where(used, trans, pltpu.roll(buoy, 4, 0))

    pl.semaphore_wait(barrier, 7 + 2 * here.parity)

    @pl.when(here.parity == 1)
    def _():
        for neighbour in both_sides:
            pl.semaphore_signal(ready, inc=1, device_id=neighbour, device_id_type=MESH)

    def part_copy(m, pair):
        return pltpu.make_async_remote_copy(
            tiles.at[pair], parts.at[m], part_send.at[pair], part_recv.at[m],
            device_id=peer(OTHERS[m]), device_id_type=MESH,
        )

    for m, other in enumerate(OTHERS):
        for pair, owner in ((0, 0), (1, 7)):

            @pl.when(here.order_of(other) == owner)
            def _(m=m, pair=pair):
                part_copy(m, pair).start()

    for m, other in enumerate(OTHERS):
        copy = pltpu.make_async_remote_copy(
            thick_all.at[layer], thick_all.at[layer], th_send.at[m], th_recv.at[m],
            device_id=peer(other), device_id_type=MESH,
        )
        copy.start()
        waits.append(copy)

    def conduct_slab(n, h, flip):
        for copy in loads[n]:
            copy.wait()
        start = here.base(h, flip)

        @pl.loop(0, SLAB // 8)
        def _(i):
            rows = pl.ds(pl.multiple_of(start + i * 8, 8), 8)
            top = capv[rows, :]
            bottom = pluv[rows, :]
            trans = None
            for k in range(LAYERS):
                depth = layer * LAYERS + k
                flow = permv[k, rows, :] * mobv[k, rows, :] * thick_s[k]
                flow = jnp.where(depth >= top, flow, 0.0)
                cond[k, rows, :] = flow
                part = jnp.where(depth < bottom, flow, 0.0)
                trans, buoy = (flow, part) if trans is None else (trans + flow, buoy + part)
            tb[0, rows, :] = trans
            tb[1, rows, :] = buoy

    def rs_copy(h, q, number, rows, buffer, dim):
        return pltpu.make_async_remote_copy(
            tb.at[:, rows], buffer, rs_send.at[3 * h + q, number], rs_recv.at[3 * h + q, number],
            device_id=peer(flip_of(dim)), device_id_type=MESH,
        )

    PIECES = ((1, 1), (1, 0), (0, 1), (0, 0))

    def part_rows(h, q, flip):
        return here.rows(h, flip, PART_START[h][q], PART_ROWS[h][q])

    def first_copy(h, q, n):
        d1, d2, d3 = ORDERS[q]
        e2, e3 = PIECES[n]
        flip = flip_of(*([d1] + [d2] * e2 + [d3] * e3))
        return flip, rs_copy(h, q, n, part_rows(h, q, flip), r1[h][q].at[n], d1)

    def second_copy(h, q, n):
        d1, d2, d3 = ORDERS[q]
        flip = flip_of(*([d2] + ([d3] if n == 0 else [])))
        return rs_copy(h, q, 4 + n, part_rows(h, q, flip), r2[h][q].at[n], d2), flip

    def third_copy(h, q):
        flip = flip_of(ORDERS[q][2])
        return rs_copy(h, q, 6, part_rows(h, q, flip), r3[h][q], ORDERS[q][2]), flip

    def send(copy):
        copy.start()
        waits.append(copy)

    later = []
    for n, (h, flip) in enumerate(blocks):
        conduct_slab(n, h, flip)
        for q in range(3):
            for m in range(4):
                owner, copy = first_copy(h, q, m)
                if owner == flip:
                    if h == 0 or m < 2:
                        send(copy)
                    else:
                        later.append(copy)

    def row_copy(n, array):
        return pltpu.make_async_remote_copy(
            array.at[:, pl.ds(0, 8)], array.at[:, pl.ds(ROWS, 8)], row_send.at[n], row_recv.at[n],
            device_id=(area - 1, layer), device_id_type=MESH,
        )

    def across(tile):
        return jnp.concatenate([tile] * (COLS // 128), axis=1)

    def gas_sum(blocks, top, bottom):
        def lookup(index, count):
            def step(block, found):
                for k in range(LAYERS):
                    depth = block * LAYERS + k
                    found = jnp.where(depth < index, across(table[depth + 1]), found)
                return found

            return lax.fori_loop(0, count, step, jnp.zeros(index.shape, jnp.float32))

        return jnp.maximum(lookup(bottom, blocks) - lookup(top, jnp.minimum(blocks, 4)), 0.0)

    def heads(low, high):
        @pl.loop(low, high)
        def _(i):
            rows = pl.ds(pl.multiple_of(i * 8, 8), 8)
            top = capv[rows, :]
            bottom = pluv[rows, :]
            above = across(table[layer * LAYERS]) - (brine_density - gas_density) * gas_sum(layer, top, bottom)
            for k in range(LAYERS):
                depth = layer * LAYERS + k
                inside = (depth >= top) & (depth < bottom)
                mass = jnp.where(inside, gas_density * thick_s[k], brine_density * thick_s[k])
                hh[k, rows, :] = gravity_scale * (above + 0.5 * mass)
                above = above + mass

    lane_last = lax.broadcasted_iota(jnp.int32, (32, COLS), 1) < COLS - 1

    def faces(low, high):
        @pl.loop(low * LAYERS, high * LAYERS)
        def _(i):
            k = i % LAYERS
            start = pl.multiple_of((i // LAYERS) * 32, 8)
            flow = cond[k, pl.ds(start, 40), :]
            head = hh[k, pl.ds(start, 40), :]
            next_flow = pltpu.roll(flow, 39, 0)[:32]
            next_head = pltpu.roll(head, 39, 0)[:32]
            flow = flow[:32]
            head = head[:32]
            rows = pl.ds(start, 32)
            face = harmonic(flow, next_flow)
            hr[k, rows, :] = face
            gr[k, rows, :] = face * (head - next_head)
            side_flow = jnp.where(lane_last, pltpu.roll(flow, COLS - 1, 1), 0.0)
            side_head = pltpu.roll(head, COLS - 1, 1)
            face = harmonic(flow, side_flow)
            hc[k, rows, :] = face
            gc[k, rows, :] = face * (head - side_head)

    def second(h, n):
        for q in range(3):
            first_copy(h, q, n)[1].wait_recv()
            copy, flip = second_copy(h, q, n)
            rows = part_rows(h, q, flip)
            tb[:, rows, :] = tb[:, rows, :] + r1[h][q][n]
            send(copy)

    def third(h):
        for q in range(3):
            first_copy(h, q, 2)[1].wait_recv()
            second_copy(h, q, 0)[0].wait_recv()
            copy, flip = third_copy(h, q)
            rows = part_rows(h, q, flip)
            tb[:, rows, :] = tb[:, rows, :] + (r1[h][q][2] + r2[h][q][0])
            send(copy)

    def final(h):
        for q in range(3):
            first_copy(h, q, 3)[1].wait_recv()
            second_copy(h, q, 1)[0].wait_recv()
            third_copy(h, q)[0].wait_recv()
            mine = part_rows(h, q, OWN)
            at = pl.ds(HALO + PART_START[h][q], PART_ROWS[h][q])
            wide[h, :, at, :] = tb[:, mine, :] + r1[h][q][3] + (r2[h][q][1] + r3[h][q][...])

    forward_up = pltpu.make_async_remote_copy(
        sums.at[0], cross.at[1], sum_send.at[0], sum_recv.at[1],
        device_id=(area - 1, layer), device_id_type=MESH,
    )
    forward_down = pltpu.make_async_remote_copy(
        sums.at[1], cross.at[0], sum_send.at[1], sum_recv.at[0],
        device_id=(area + 1, layer), device_id_type=MESH,
    )

    def forward_edges():
        for owned, pair in ((at_ends, 0), (at_middle, 1)):

            @pl.when(owned)
            def _(pair=pair):
                for m in range(7):
                    part_copy(m, pair).wait_recv()
                total = tiles[pair]
                for m in range(7):
                    total = total + parts[m]
                sums[...] = total

        @pl.when(crosses_up)
        def _():
            for copy in (forward_up, *to_up):
                copy.start()

        @pl.when(crosses_down)
        def _():
            for copy in (forward_down, *to_down):
                copy.start()

        @pl.when(area > 0)
        def _():
            row_copy(0, cond).start()

    def gas_rows(h, at):
        rows = pl.ds(at, 8)
        gas[h, rows, :] = buoyancy_scale * gas_sum(8, edge_i[h, 0, rows, :], edge_i[h, 1, rows, :])

    def halo_copies(h):
        before_layer = here.layer_at(jnp.maximum(here.order - 1, 0))
        after_layer = here.layer_at(jnp.minimum(here.order + 1, 7))
        inner = pltpu.make_async_remote_copy(
            wide.at[h, :, pl.ds(SLAB if h else HALO, HALO)],
            wide.at[h, :, pl.ds(0 if h else HALO + SLAB, HALO)],
            halo_send.at[h, 0], halo_recv.at[h, 0], device_id=(area, before_layer), device_id_type=MESH,
        )
        outer = pltpu.make_async_remote_copy(
            wide.at[h, :, pl.ds(HALO if h else SLAB, HALO)],
            wide.at[h, :, pl.ds(HALO + SLAB if h else 0, HALO)],
            halo_send.at[h, 1], halo_recv.at[h, 1], device_id=(area, after_layer), device_id_type=MESH,
        )
        return inner, outer

    def halo_start(h):
        inner, outer = halo_copies(h)

        @pl.when(here.order > 0)
        def _():
            inner.start()

        @pl.when(here.order < 7)
        def _():
            outer.start()

    def blank(h, at):
        rows = pl.ds(at, HALO)
        edge_i[h, :, rows, :] = jnp.zeros((2, HALO, COLS), jnp.int32)
        edge_f[h, 0, rows, :] = jnp.ones((HALO, COLS), jnp.float32)
        edge_f[h, 1, rows, :] = jnp.zeros((HALO, COLS), jnp.float32)
        edge_f[h, 2, rows, :] = jnp.zeros((HALO, COLS), jnp.float32)
        wide[h, :, rows, :] = jnp.zeros((2, HALO, COLS), jnp.float32)

    def unpack(h, at, tile, used):
        rows = pl.ds(at, HALO)
        wide[h, 0, rows, :] = jnp.where(used, tile, 0.0)
        wide[h, 1, rows, :] = jnp.where(used, pltpu.roll(tile, 4, 0), 0.0)

    def halo_finish(h):
        inner, outer = halo_copies(h)
        if h == 0:

            @pl.when(top_edge)
            def _():
                blank(0, 0)

            @pl.when(crosses_up)
            def _():
                for copy in (forward_down, *to_down):
                    copy.wait_recv()
                unpack(0, 0, cross[0], sub8 >= 4)

            @pl.when(at_middle)
            def _():
                unpack(0, HALO + SLAB, sums[0], sub8 < 4)

            gas_rows(0, 0)
        else:

            @pl.when(bottom_edge)
            def _():
                blank(1, HALO + SLAB)

            @pl.when(crosses_down)
            def _():
                for copy in (forward_up, *to_up):
                    copy.wait_recv()
                unpack(1, HALO + SLAB, cross[1], sub8 < 4)

            @pl.when(at_middle)
            def _():
                unpack(1, 0, sums[1], sub8 >= 4)

            gas_rows(1, HALO + SLAB)

        @pl.when(here.order > 0)
        def _():
            outer.wait_recv()

        @pl.when(here.order < 7)
        def _():
            inner.wait_recv()

    lane = lax.broadcasted_iota(jnp.int32, (WIDE, COLS), 1)

    def after(x):
        return pltpu.roll(x, WIDE - 1, 0)

    def before(x):
        return pltpu.roll(x, 1, 0)

    def right(x):
        return jnp.where(lane < COLS - 1, pltpu.roll(x, COLS - 1, 1), 0.0)

    def left(x):
        return jnp.where(lane > 0, pltpu.roll(x, 1, 1), 0.0)

    def relax(h):
        trans = wide[h, 0]
        face_row = harmonic(trans, after(trans))
        t_row[...] = face_row
        face_col = harmonic(trans, right(trans))
        t_col[...] = face_col
        diagonal = edge_f[h, 0] + face_row + before(face_row) + face_col + left(face_col)
        inverse[...] = 1.0 / diagonal
        buoy = wide[h, 1]
        drive = gas[h]
        push = harmonic(buoy, after(buoy)) * (after(drive) - drive)
        total = push - before(push)
        push = harmonic(buoy, right(buoy)) * (right(drive) - drive)
        total = total + (push - left(push))
        right_hand[...] = edge_f[h, 0] * edge_f[h, 2] + edge_f[h, 1] + total

        for sweep in range(SWEEPS):
            pressure = edge_f[h, 2]
            face_row = t_row[...]
            face_col = t_col[...]
            inflow = face_row * after(pressure) + before(face_row * pressure)
            inflow = inflow + (face_col * right(pressure) + left(face_col * pressure))
            edge_f[h, 2] = (right_hand[...] + inflow) * inverse[...]

        pf[here.rows(h, OWN, 0, SLAB), :] = edge_f[h, 2, pl.ds(HALO, SLAB), :]

    def ag_messages(h):
        def first_rows(flip):
            return here.rows(h, flip, 0, X_FIRST[h])

        def later_rows(flip):
            return here.rows(h, flip, X_FIRST[h], SLAB - X_FIRST[h])

        half_x = (0, first_rows, OWN, OTHER_HALF)
        x_own = [(1 + n, later_rows, OWN, x) for n, x in enumerate(ACROSS)]
        x_first = [(4 + n, first_rows, OWN, x) for n, x in enumerate(ACROSS)]
        half_own = (7, later_rows, OWN, OTHER_HALF)
        half_on = [(8 + n, first_rows, OTHER_HALF, x) for n, x in enumerate(ACROSS)]
        x_on = [(11 + n, later_rows, x, OTHER_HALF) for n, x in enumerate(ACROSS)]
        return half_x, x_own, x_first, half_own, half_on, x_on

    def ag_copy(h, number, rows, to):
        return pltpu.make_async_remote_copy(
            pf.at[rows], pf.at[rows], ag_send.at[h, number], ag_recv.at[h, number],
            device_id=peer(to), device_id_type=MESH,
        )

    def spread(h, number, rows_of, flip, to):
        send(ag_copy(h, number, rows_of(flip), to))

    def arrived(h, number, rows_of, flip, to):
        ag_copy(h, number, rows_of(plus(flip, to)), to).wait_recv()

    def gather_start(h):
        half_x, x_own, x_first, half_own, _, _ = ag_messages(h)
        for message in (half_x, *x_own, *x_first, half_own):
            spread(h, *message)

    def gather_pass(h):
        half_x, x_own, _, _, half_on, x_on = ag_messages(h)
        arrived(h, *half_x)
        for n in range(3):
            spread(h, *half_on[n])
        for n in (1, 2, 0):
            arrived(h, *x_own[n])
            spread(h, *x_on[n])

    def gather_finish(h):
        _, _, x_first, half_own, half_on, x_on = ag_messages(h)
        for message in (*x_first, half_own, *half_on, *x_on):
            arrived(h, *message)

    def last_copy(m, other):
        return pltpu.make_async_remote_copy(
            pf.at[pl.ds(ROWS, 8)], pf.at[pl.ds(ROWS, 8)], last_send.at[m], last_recv.at[0],
            device_id=peer(other), device_id_type=MESH,
        )

    second(0, 0)
    second(0, 1)
    for copy in later:
        send(copy)

    for m, other in enumerate(OTHERS):
        pltpu.make_async_remote_copy(
            thick_all.at[layer], thick_all.at[here.layer_of(other)], th_send.at[m], th_recv.at[m],
            device_id=peer(other), device_id_type=MESH,
        ).wait_recv()
    total = jnp.zeros((8, 128), jnp.float32)
    table[0] = total
    for block in range(8):
        for k in range(LAYERS):
            total = total + jnp.broadcast_to(thick_all[block, pl.ds(k, 1), :], (8, 128))
            table[block * LAYERS + k + 1] = total


    third(0)
    second(1, 0)
    second(1, 1)

    @pl.when(here.parity == 0)
    def _():
        pl.semaphore_wait(ready, 2)

    forward_edges()
    heads(0, 32)

    for copy in (*always[0], *always[1]):
        copy.wait()

    @pl.when(here.order > 0)
    def _():
        for h in range(HALVES):
            for copy in sometimes(h):
                copy.wait()

    @pl.loop(1, WIDE // 8)
    def _(i):
        gas_rows(0, pl.multiple_of(i * 8, 8))

    final(0)
    halo_start(0)
    third(1)

    @pl.loop(0, WIDE // 8 - 1)
    def _(i):
        gas_rows(1, pl.multiple_of(i * 8, 8))

    halo_finish(0)
    relax(0)
    gather_start(0)
    heads(32, 64)

    @pl.when(area > 0)
    def _():
        row_copy(1, hh).start()

    final(1)
    halo_start(1)
    gather_pass(0)
    halo_finish(1)
    relax(1)
    gather_start(1)

    @pl.when(at_ends)
    def _():
        pf[pl.ds(ROWS, 8), :] = edge_f[1, 2, pl.ds(HALO + SLAB, 8), :]
        for m, other in enumerate(OTHERS):
            last_copy(m, other).start()

    faces(0, 7)
    gather_pass(1)
    faces(7, 15)

    @pl.when(area < here.areas - 1)
    def _():
        row_copy(0, cond).wait_recv()
        row_copy(1, hh).wait_recv()

    @pl.when(area == here.areas - 1)
    def _():
        cond[:, pl.ds(ROWS, 8), :] = jnp.zeros((LAYERS, 8, COLS), jnp.float32)
        hh[:, pl.ds(ROWS, 8), :] = jnp.zeros((LAYERS, 8, COLS), jnp.float32)

    faces(15, 16)
    gather_finish(0)
    gather_finish(1)

    @pl.when(here.order > 0)
    def _():
        last_copy(0, OTHERS[0]).wait_recv()

    for copy in waits:
        copy.wait_send()

    @pl.when(at_ends)
    def _():
        for m, other in enumerate(OTHERS):
            last_copy(m, other).wait_send()

    for h in range(HALVES):
        inner, outer = halo_copies(h)

        @pl.when(here.order > 0)
        def _(inner=inner):
            inner.wait_send()

        @pl.when(here.order < 7)
        def _(outer=outer):
            outer.wait_send()

    @pl.when(here.order > 0)
    def _():
        part_copy(0, 0).wait_send()

    @pl.when(here.order < 7)
    def _():
        part_copy(0, 1).wait_send()

    @pl.when(area > 0)
    def _():
        row_copy(0, cond).wait_send()
        row_copy(1, hh).wait_send()

    @pl.when(crosses_up)
    def _():
        for copy in (forward_up, *to_up):
            copy.wait_send()

    @pl.when(crosses_down)
    def _():
        for copy in (forward_down, *to_down):
            copy.wait_send()


CHUNK = 32


def write_kernel(hh, hr, gr, hc, gc, pf, cell, rows_out, cols_out, cell_v, rows_v, cols_v, sems):
    chunks = ROWS // CHUNK

    def copies(i):
        rows = pl.ds(pl.multiple_of(i * CHUNK, 8), CHUNK)
        return [
            pltpu.make_async_copy(v.at[:, rows], o.at[:, rows], sems.at[n, i])
            for n, (v, o) in enumerate(((cell_v, cell), (rows_v, rows_out), (cols_v, cols_out)))
        ]

    @pl.loop(0, chunks)
    def _(i):
        start = pl.multiple_of(i * CHUNK, 8)
        rows = pl.ds(start, CHUNK)
        wide = pf[pl.ds(start, CHUNK + 8), :]
        pressure = wide[:CHUNK]
        row_drop = pressure - pltpu.roll(wide, CHUNK + 7, 0)[:CHUNK]
        col_drop = pressure - pltpu.roll(pressure, COLS - 1, 1)
        for k in range(LAYERS):
            cell_v[k, rows, :] = pressure + hh[k, rows, :]
            rows_v[k, rows, :] = hr[k, rows, :] * row_drop + gr[k, rows, :]
            cols_v[k, rows, :] = hc[k, rows, :] * col_drop + gc[k, rows, :]
        for copy in copies(i):
            copy.start()

    @pl.loop(0, chunks)
    def _(i):
        for copy in copies(i):
            copy.wait()


def local(permeability, mobility, thickness, caprock, plume, storage, source, pressure_old):
    f32, i32 = jnp.float32, jnp.int32
    vmem = pl.BlockSpec(memory_space=pltpu.VMEM)
    hbm = pl.BlockSpec(memory_space=pltpu.HBM)
    dma = pltpu.SemaphoreType.DMA
    V = pltpu.VMEM
    full = V((LAYERS, ROWS, COLS), f32)
    tall = V((LAYERS, ROWS + 8, COLS), f32)
    arrays = (permeability, mobility, thickness, caprock, plume, storage, source, pressure_old)
    arrays = [pltpu.with_memory_space_constraint(x, pltpu.HBM) for x in arrays]
    kept = pl.pallas_call(
        gather_kernel,
        out_shape=[tall, full, full, full, full, V((ROWS + 8, COLS), f32)],
        in_specs=[hbm] * 8,
        out_specs=[vmem] * 6,
        scratch_shapes=[
            *[V((4, 2, r, COLS), f32) for parts in PART_ROWS for r in parts],
            *[V((2, 2, r, COLS), f32) for parts in PART_ROWS for r in parts],
            *[V((2, r, COLS), f32) for parts in PART_ROWS for r in parts],
            V((LAYERS, ROWS, COLS), f32), V((LAYERS, ROWS, COLS), f32), V((LAYERS, ROWS + 8, COLS), f32),
            V((ROWS, COLS), i32), V((ROWS, COLS), i32), V((2, ROWS, COLS), f32),
            V((2, 4, LAYERS, 8, COLS), f32), V((2, 4, 8, COLS), i32), V((2, 2, 8, COLS), f32),
            V((7, 2, 8, COLS), f32), V((2, 8, COLS), f32), V((2, 8, COLS), f32),
            V((HALVES, 2, WIDE, COLS), f32), V((HALVES, 2, WIDE, COLS), i32), V((HALVES, 3, WIDE, COLS), f32),
            pltpu.SMEM((LAYERS,), f32), V((8, 8, 128), f32), V((33, 8, 128), f32),
            V((HALVES, WIDE, COLS), f32), *[V((WIDE, COLS), f32) for _ in range(4)],
            dma((16, 4)), dma((4, 5)), dma((1,)), dma((6, 7)), dma((6, 7)), dma((2, 14)), dma((2, 14)),
            dma((7,)), dma((7,)),
            dma((4, 4)), dma((2,)), dma((7,)), dma((2,)), dma((2,)), pltpu.SemaphoreType.REGULAR,
            dma((2, 2)), dma((2, 2)), dma((2, 5)), dma((2, 5)), dma((2,)), dma((2,)),
            dma((7,)), dma((1,)),
        ],
        compiler_params=pltpu.CompilerParams(
            collective_id=0, has_side_effects=True, vmem_limit_bytes=26 << 20
        ),
        name="gather",
    )(*arrays)
    return pl.pallas_call(
        write_kernel,
        out_shape=[jax.ShapeDtypeStruct((LAYERS, ROWS, COLS), f32)] * 3,
        in_specs=[vmem] * 6,
        out_specs=[hbm] * 3,
        scratch_shapes=[V((LAYERS, ROWS, COLS), f32)] * 3 + [dma((3, ROWS // CHUNK))],
        compiler_params=pltpu.CompilerParams(vmem_limit_bytes=16 << 20),
        name="write",
    )(*kept)


def solution(mesh):
    in_specs = (
        P("layer", "area", None),
        P("layer", "area", None),
        P("layer"),
        P("area", None),
        P("area", None),
        P("area", None),
        P("area", None),
        P("area", None),
    )
    out_specs = (P("layer", "area", None), P("layer", "area", None), P("layer", "area", None))
    return jax.shard_map(
        lambda *args: tuple(local(*args)), mesh=mesh, in_specs=in_specs, out_specs=out_specs, check_vma=False
    )
```

```python
import functools

import jax
import jax.numpy as jnp
from jax import lax
from jax.experimental import pallas as pl
from jax.experimental.pallas import tpu as pltpu
from jax.sharding import PartitionSpec as P

SWEEPS = 3
buoyancy_scale = 0.3
gravity_scale = 0.05
gas_density = 0.7
brine_density = 1.0

LAYERS = 4
ROWS = 512
COLS = 512
SLAB = 64
HALO = 8
WIDE = SLAB + 2 * HALO
MESH = pl.DeviceIdType.MESH

ORDERS = ((0, 1, 2), (1, 2, 0), (2, 0, 1))
PART_START = (0, 24, 48)
PART_ROWS = (24, 24, 16)
FLIPS = ((1, 1, 1), (1, 1, 0), (0, 1, 1), (1, 0, 1), (1, 0, 0), (0, 1, 0), (0, 0, 1), (0, 0, 0))
OTHERS = FLIPS[:-1]
X_FIRST = 24
ACROSS = ((1, 1, 0), (1, 0, 0), (0, 1, 0))
OTHER_HALF = (0, 0, 1)
OWN = (0, 0, 0)


def harmonic(near_value, far_value):
    summed = near_value + far_value
    divisor = jnp.where(summed > 0, summed, 1.0)
    return 2.0 * near_value * far_value / divisor


def flip_of(*dims):
    return tuple(1 if d in dims else 0 for d in range(3))


def plus(one, two):
    return tuple((a + b) % 2 for a, b in zip(one, two))


class Place:
    def __init__(self):
        self.area = lax.axis_index("area")
        self.layer = lax.axis_index("layer")
        self.areas = lax.axis_size("area")
        x = self.layer % 4
        second = x // 2
        first = (x % 2) + second - 2 * (x % 2) * second
        self.code = (first, second, self.layer // 4)
        self.parity = self.area % 2
        self.slab = self.slab_of((0, 0, 0))

    def flipped(self, flip):
        return tuple((1 - c) if f else c for c, f in zip(self.code, flip))

    def layer_of(self, flip):
        first, second, half = self.flipped(flip)
        x = 2 * second + first + second - 2 * first * second
        return half * 4 + x

    def slab_of(self, flip):
        first, second, half = self.flipped(flip)
        x = 2 * second + first + second - 2 * first * second
        order = x + half * (7 - 2 * x)
        return order + self.parity * (7 - 2 * order)

    def layer_of_slab(self, slab):
        order = slab + self.parity * (7 - 2 * slab)
        return order + (order // 4) * (11 - 2 * order)

    def rows(self, flip, start, count):
        return pl.ds(pl.multiple_of(self.slab_of(flip) * SLAB + start, 8), count)


def gather_kernel(
    perm, mob, thick, cap, plu, sto, src, old,
    hh, hr, gr, hc, gc, pf,
    permv, mobv, cond, capv, pluv, tb, r1a, r1b, r1c, r2a, r2b, r2c, r3a, r3b, r3c,
    edge_3d, edge_2d, tiles, parts, sums, cross,
    wide, edge_i, edge_f, thick_s, thick_all, table, gas, t_row, t_col, right_hand, inverse,
    in_sem, edge_sem, thick_sem, rs_send, rs_recv, ag_send, ag_recv, th_send, th_recv,
    part_load, part_send, part_recv, sum_send, sum_recv, ready,
    halo_send, halo_recv, input_send, input_recv, row_send, row_recv, last_send, last_recv,
):
    here = Place()
    area, layer = here.area, here.layer
    r1, r2, r3 = (r1a, r1b, r1c), (r2a, r2b, r2c), (r3a, r3b, r3c)
    waits = []
    is_first = here.slab == 0
    is_last = here.slab == 7

    def peer(flip):
        return (area, here.layer_of(flip))

    loads = []
    thick_copy = pltpu.make_async_copy(thick, thick_s, thick_sem.at[0])
    thick_copy.start()
    part_copies = []
    for side, first_row in ((0, 0), (1, ROWS - HALO)):
        rows = pl.ds(first_row, HALO)
        part_copies += [
            pltpu.make_async_copy(cap.at[rows], edge_2d.at[0, side], part_load.at[side, 0]),
            pltpu.make_async_copy(plu.at[rows], edge_2d.at[1, side], part_load.at[side, 1]),
            pltpu.make_async_copy(perm.at[:, rows], edge_3d.at[0, side], part_load.at[side, 2]),
            pltpu.make_async_copy(mob.at[:, rows], edge_3d.at[1, side], part_load.at[side, 3]),
        ]
    for copy in part_copies:
        copy.start()
    for n, flip in enumerate(FLIPS):
        rows = here.rows(flip, 0, SLAB)
        group = [
            pltpu.make_async_copy(cap.at[rows], capv.at[rows], in_sem.at[n, 0]),
            pltpu.make_async_copy(plu.at[rows], pluv.at[rows], in_sem.at[n, 1]),
            pltpu.make_async_copy(perm.at[:, rows], permv.at[:, rows], in_sem.at[n, 2]),
            pltpu.make_async_copy(mob.at[:, rows], mobv.at[:, rows], in_sem.at[n, 3]),
        ]
        for copy in group:
            copy.start()
        loads.append(group)

    barrier = pltpu.get_barrier_semaphore()
    for flip in OTHERS:
        pl.semaphore_signal(barrier, inc=1, device_id=peer(flip), device_id_type=MESH)
    both_sides = [((area + step) % here.areas, layer) for step in (1, here.areas - 1)]

    @pl.when(here.parity == 0)
    def _():
        for neighbour in both_sides:
            pl.semaphore_signal(barrier, inc=1, device_id=neighbour, device_id_type=MESH)

    base = here.slab * SLAB
    sources = (cap, plu, sto, src, old)
    targets = (edge_i.at[0], edge_i.at[1], edge_f.at[0], edge_f.at[1], edge_f.at[2])

    def edge_copies(sem_row, first_row, count, at):
        rows = pl.ds(pl.multiple_of(base + first_row, 8), count)
        return [
            pltpu.make_async_copy(s.at[rows], t.at[pl.ds(at, count)], edge_sem.at[sem_row, n])
            for n, (s, t) in enumerate(zip(sources, targets))
        ]

    mid_copies = edge_copies(0, 0, SLAB, HALO)
    for copy in mid_copies:
        copy.start()

    @pl.when(here.slab > 0)
    def _():
        for copy in edge_copies(1, -HALO, HALO, 0):
            copy.start()

    @pl.when(here.slab < 7)
    def _():
        for copy in edge_copies(2, SLAB, HALO, HALO + SLAB):
            copy.start()

    thick_copy.wait()
    sublane = lax.broadcasted_iota(jnp.int32, (8, 128), 0)
    tile = jnp.zeros((8, 128), jnp.float32)
    for k in range(LAYERS):
        tile = jnp.where(sublane == k, thick_s[k], tile)
    thick_all[layer] = tile

    def input_sends():
        up = [
            pltpu.make_async_remote_copy(
                s.at[pl.ds(0, HALO)], t.at[pl.ds(HALO + SLAB, HALO)],
                input_send.at[0, n], input_recv.at[0, n],
                device_id=(area - 1, layer), device_id_type=MESH,
            )
            for n, (s, t) in enumerate(zip(sources, targets))
        ]
        down = [
            pltpu.make_async_remote_copy(
                s.at[pl.ds(ROWS - HALO, HALO)], t.at[pl.ds(0, HALO)],
                input_send.at[1, n], input_recv.at[1, n],
                device_id=(area + 1, layer), device_id_type=MESH,
            )
            for n, (s, t) in enumerate(zip(sources, targets))
        ]
        return up, down

    to_up, to_down = input_sends()
    crosses_up = is_first & (area > 0)
    crosses_down = is_last & (area < here.areas - 1)
    top_edge = is_first & (area == 0)
    bottom_edge = is_last & (area == here.areas - 1)

    sub8 = lax.broadcasted_iota(jnp.int32, (8, COLS), 0)
    for copy in part_copies:
        copy.wait()
    for side in (0, 1):
        top = edge_2d[0, side]
        bottom = edge_2d[1, side]
        trans = buoy = jnp.zeros((8, COLS), jnp.float32)
        for k in range(LAYERS):
            depth = layer * LAYERS + k
            flow = edge_3d[0, side, k] * edge_3d[1, side, k] * thick_s[k]
            flow = jnp.where(depth >= top, flow, 0.0)
            trans = trans + flow
            buoy = buoy + jnp.where(depth < bottom, flow, 0.0)
        used = (sub8 < 4) if side == 0 else (sub8 >= 4)
        tiles[side] = jnp.where(used, trans, pltpu.roll(buoy, 4, 0))

    pl.semaphore_wait(barrier, 7 + 2 * here.parity)

    @pl.when(here.parity == 1)
    def _():
        for neighbour in both_sides:
            pl.semaphore_signal(ready, inc=1, device_id=neighbour, device_id_type=MESH)

    def part_copy(m, side):
        return pltpu.make_async_remote_copy(
            tiles.at[side], parts.at[m], part_send.at[side], part_recv.at[m],
            device_id=peer(OTHERS[m]), device_id_type=MESH,
        )

    for m, other in enumerate(OTHERS):
        for side, owner in ((0, 0), (1, 7)):

            @pl.when(here.slab_of(other) == owner)
            def _(m=m, side=side):
                part_copy(m, side).start()

    for m, other in enumerate(OTHERS):
        copy = pltpu.make_async_remote_copy(
            thick_all.at[layer], thick_all.at[layer], th_send.at[m], th_recv.at[m],
            device_id=peer(other), device_id_type=MESH,
        )
        copy.start()
        waits.append(copy)

    def conduct_slab(n, flip):
        for copy in loads[n]:
            copy.wait()
        start = here.slab_of(flip) * SLAB

        @pl.loop(0, SLAB // 8)
        def _(i):
            rows = pl.ds(pl.multiple_of(start + i * 8, 8), 8)
            top = capv[rows, :]
            bottom = pluv[rows, :]
            trans = None
            for k in range(LAYERS):
                depth = layer * LAYERS + k
                flow = permv[k, rows, :] * mobv[k, rows, :] * thick_s[k]
                flow = jnp.where(depth >= top, flow, 0.0)
                cond[k, rows, :] = flow
                part = jnp.where(depth < bottom, flow, 0.0)
                trans, buoy = (flow, part) if trans is None else (trans + flow, buoy + part)
            tb[0, rows, :] = trans
            tb[1, rows, :] = buoy

    def rs_copy(q, number, rows, buffer, dim):
        return pltpu.make_async_remote_copy(
            tb.at[:, rows], buffer, rs_send.at[q, number], rs_recv.at[q, number],
            device_id=peer(flip_of(dim)), device_id_type=MESH,
        )

    PIECES = ((1, 1), (1, 0), (0, 1), (0, 0))

    def part_rows(q, flip):
        return here.rows(flip, PART_START[q], PART_ROWS[q])

    def first_copy(q, n):
        d1, d2, d3 = ORDERS[q]
        e2, e3 = PIECES[n]
        flip = flip_of(*([d1] + [d2] * e2 + [d3] * e3))
        return flip, rs_copy(q, n, part_rows(q, flip), r1[q].at[n], d1)

    def second_copy(q, n):
        d1, d2, d3 = ORDERS[q]
        flip = flip_of(*([d2] + ([d3] if n == 0 else [])))
        return flip, rs_copy(q, 4 + n, part_rows(q, flip), r2[q].at[n], d2)

    def third_copy(q):
        d1, d2, d3 = ORDERS[q]
        flip = flip_of(d3)
        return flip, rs_copy(q, 6, part_rows(q, flip), r3[q], d3)

    for n, flip in enumerate(FLIPS):
        conduct_slab(n, flip)
        for q in range(3):
            for m in range(4):
                owner, copy = first_copy(q, m)
                if owner == flip:
                    copy.start()
                    waits.append(copy)

    def row_copy(n, array):
        return pltpu.make_async_remote_copy(
            array.at[:, pl.ds(0, 8)], array.at[:, pl.ds(ROWS, 8)], row_send.at[n], row_recv.at[n],
            device_id=(area - 1, layer), device_id_type=MESH,
        )

    def across(tile):
        return jnp.concatenate([tile] * (COLS // 128), axis=1)

    def gas_sum(blocks, top, bottom):
        def lookup(index, count):
            def step(block, found):
                for k in range(LAYERS):
                    depth = block * LAYERS + k
                    found = jnp.where(depth < index, across(table[depth + 1]), found)
                return found

            return lax.fori_loop(0, count, step, jnp.zeros(index.shape, jnp.float32))

        return jnp.maximum(lookup(bottom, blocks) - lookup(top, jnp.minimum(blocks, 4)), 0.0)

    def heads(low, high):
        @pl.loop(low, high)
        def _(i):
            rows = pl.ds(pl.multiple_of(i * 8, 8), 8)
            top = capv[rows, :]
            bottom = pluv[rows, :]
            above = across(table[layer * LAYERS]) - (brine_density - gas_density) * gas_sum(layer, top, bottom)
            for k in range(LAYERS):
                depth = layer * LAYERS + k
                inside = (depth >= top) & (depth < bottom)
                mass = jnp.where(inside, gas_density * thick_s[k], brine_density * thick_s[k])
                hh[k, rows, :] = gravity_scale * (above + 0.5 * mass)
                above = above + mass

    lane_last = lax.broadcasted_iota(jnp.int32, (32, COLS), 1) < COLS - 1

    def faces(low, high):
        @pl.loop(low * LAYERS, high * LAYERS)
        def _(i):
            k = i % LAYERS
            start = pl.multiple_of((i // LAYERS) * 32, 8)
            flow = cond[k, pl.ds(start, 40), :]
            head = hh[k, pl.ds(start, 40), :]
            next_flow = pltpu.roll(flow, 39, 0)[:32]
            next_head = pltpu.roll(head, 39, 0)[:32]
            flow = flow[:32]
            head = head[:32]
            rows = pl.ds(start, 32)
            face = harmonic(flow, next_flow)
            hr[k, rows, :] = face
            gr[k, rows, :] = face * (head - next_head)
            side_flow = jnp.where(lane_last, pltpu.roll(flow, COLS - 1, 1), 0.0)
            side_head = pltpu.roll(head, COLS - 1, 1)
            face = harmonic(flow, side_flow)
            hc[k, rows, :] = face
            gc[k, rows, :] = face * (head - side_head)

    def second(n):
        for q in range(3):
            _, arrived = first_copy(q, n)
            arrived.wait_recv()
            flip, copy = second_copy(q, n)
            rows = part_rows(q, flip)
            tb[:, rows, :] = tb[:, rows, :] + r1[q][n]
            copy.start()
            waits.append(copy)

    forward_up = pltpu.make_async_remote_copy(
        sums, cross.at[1], sum_send.at[0], sum_recv.at[1],
        device_id=(area - 1, layer), device_id_type=MESH,
    )
    forward_down = pltpu.make_async_remote_copy(
        sums, cross.at[0], sum_send.at[0], sum_recv.at[0],
        device_id=(area + 1, layer), device_id_type=MESH,
    )

    def forward_edges():
        for ends, side in ((is_first, 0), (is_last, 1)):

            @pl.when(ends)
            def _(side=side):
                for m in range(7):
                    part_copy(m, side).wait_recv()
                total = tiles[side]
                for m in range(7):
                    total = total + parts[m]
                sums[...] = total

        @pl.when(crosses_up)
        def _():
            for copy in (forward_up, *to_up):
                copy.start()

        @pl.when(crosses_down)
        def _():
            for copy in (forward_down, *to_down):
                copy.start()

        @pl.when(area > 0)
        def _():
            row_copy(0, cond).start()

    def gas_rows(at):
        rows = pl.ds(at, 8)
        gas[rows, :] = buoyancy_scale * gas_sum(8, edge_i[0, rows, :], edge_i[1, rows, :])

    @pl.when(here.parity == 1)
    def _():
        forward_edges()

    second(0)

    for m, other in enumerate(OTHERS):
        pltpu.make_async_remote_copy(
            thick_all.at[layer], thick_all.at[here.layer_of(other)], th_send.at[m], th_recv.at[m],
            device_id=peer(other), device_id_type=MESH,
        ).wait_recv()
    total = jnp.zeros((8, 128), jnp.float32)
    table[0] = total
    for block in range(8):
        for k in range(LAYERS):
            total = total + jnp.broadcast_to(thick_all[block, pl.ds(k, 1), :], (8, 128))
            table[block * LAYERS + k + 1] = total


    second(1)
    heads(0, 32)

    @pl.when(here.parity == 0)
    def _():
        pl.semaphore_wait(ready, 2)
        forward_edges()

    for copy in mid_copies:
        copy.wait()

    @pl.when(here.slab > 0)
    def _():
        for copy in edge_copies(1, -HALO, HALO, 0):
            copy.wait()

    @pl.when(here.slab < 7)
    def _():
        for copy in edge_copies(2, SLAB, HALO, HALO + SLAB):
            copy.wait()

    for q in range(3):
        first_copy(q, 2)[1].wait_recv()
        second_copy(q, 0)[1].wait_recv()
        flip, copy = third_copy(q)
        rows = part_rows(q, flip)
        tb[:, rows, :] = tb[:, rows, :] + (r1[q][2] + r2[q][0])
        copy.start()
        waits.append(copy)

    heads(32, 64)

    @pl.when(area > 0)
    def _():
        row_copy(1, hh).start()

    @pl.loop(1, WIDE // 8 - 1)
    def _(i):
        gas_rows(pl.multiple_of(i * 8, 8))

    for q in range(3):
        first_copy(q, 3)[1].wait_recv()
        second_copy(q, 1)[1].wait_recv()
        third_copy(q)[1].wait_recv()
        mine = part_rows(q, (0, 0, 0))
        at = pl.ds(HALO + PART_START[q], PART_ROWS[q])
        wide[:, at, :] = tb[:, mine, :] + r1[q][3] + (r2[q][1] + r3[q][...])

    up_layer = here.layer_of_slab(jnp.maximum(here.slab - 1, 0))
    down_layer = here.layer_of_slab(jnp.minimum(here.slab + 1, 7))
    halo_up = pltpu.make_async_remote_copy(
        wide.at[:, pl.ds(HALO, HALO)], wide.at[:, pl.ds(HALO + SLAB, HALO)],
        halo_send.at[0], halo_recv.at[0], device_id=(area, up_layer), device_id_type=MESH,
    )
    halo_down = pltpu.make_async_remote_copy(
        wide.at[:, pl.ds(SLAB, HALO)], wide.at[:, pl.ds(0, HALO)],
        halo_send.at[1], halo_recv.at[1], device_id=(area, down_layer), device_id_type=MESH,
    )

    @pl.when(here.slab > 0)
    def _():
        halo_up.start()

    @pl.when(here.slab < 7)
    def _():
        halo_down.start()

    def blank(at):
        rows = pl.ds(at, HALO)
        edge_i[:, rows, :] = jnp.zeros((2, HALO, COLS), jnp.int32)
        edge_f[0, rows, :] = jnp.ones((HALO, COLS), jnp.float32)
        edge_f[1, rows, :] = jnp.zeros((HALO, COLS), jnp.float32)
        edge_f[2, rows, :] = jnp.zeros((HALO, COLS), jnp.float32)
        wide[:, rows, :] = jnp.zeros((2, HALO, COLS), jnp.float32)

    def unpack(slot, at, used):
        rows = pl.ds(at, HALO)
        tile = cross[slot]
        wide[0, rows, :] = jnp.where(used, tile, 0.0)
        wide[1, rows, :] = jnp.where(used, pltpu.roll(tile, 4, 0), 0.0)

    @pl.when(top_edge)
    def _():
        blank(0)

    @pl.when(bottom_edge)
    def _():
        blank(HALO + SLAB)

    @pl.when(crosses_up)
    def _():
        for copy in (forward_down, *to_down):
            copy.wait_recv()
        unpack(0, 0, sub8 >= 4)

    @pl.when(crosses_down)
    def _():
        for copy in (forward_up, *to_up):
            copy.wait_recv()
        unpack(1, HALO + SLAB, sub8 < 4)

    gas_rows(0)
    gas_rows(HALO + SLAB)

    @pl.when(here.slab > 0)
    def _():
        halo_down.wait_recv()

    @pl.when(here.slab < 7)
    def _():
        halo_up.wait_recv()

    lane = lax.broadcasted_iota(jnp.int32, (WIDE, COLS), 1)

    def after(x):
        return pltpu.roll(x, WIDE - 1, 0)

    def before(x):
        return pltpu.roll(x, 1, 0)

    def right(x):
        return jnp.where(lane < COLS - 1, pltpu.roll(x, COLS - 1, 1), 0.0)

    def left(x):
        return jnp.where(lane > 0, pltpu.roll(x, 1, 1), 0.0)

    trans = wide[0]
    face_row = harmonic(trans, after(trans))
    t_row[...] = face_row
    face_col = harmonic(trans, right(trans))
    t_col[...] = face_col
    diagonal = edge_f[0] + face_row + before(face_row) + face_col + left(face_col)
    inverse[...] = 1.0 / diagonal
    buoy = wide[1]
    drive = gas[...]
    push = harmonic(buoy, after(buoy)) * (after(drive) - drive)
    total = push - before(push)
    push = harmonic(buoy, right(buoy)) * (right(drive) - drive)
    total = total + (push - left(push))
    right_hand[...] = edge_f[0] * edge_f[2] + edge_f[1] + total

    for sweep in range(SWEEPS):
        pressure = edge_f[2]
        face_row = t_row[...]
        face_col = t_col[...]
        inflow = face_row * after(pressure) + before(face_row * pressure)
        inflow = inflow + (face_col * right(pressure) + left(face_col * pressure))
        edge_f[2] = (right_hand[...] + inflow) * inverse[...]

    pf[here.rows((0, 0, 0), 0, SLAB), :] = edge_f[2, pl.ds(HALO, SLAB), :]

    @pl.when(is_last)
    def _():
        pf[pl.ds(ROWS, 8), :] = edge_f[2, pl.ds(HALO + SLAB, 8), :]

    def first_rows(flip):
        return here.rows(flip, 0, X_FIRST)

    def later_rows(flip):
        return here.rows(flip, X_FIRST, SLAB - X_FIRST)

    def ag_copy(number, rows, to):
        return pltpu.make_async_remote_copy(
            pf.at[rows], pf.at[rows], ag_send.at[number], ag_recv.at[number],
            device_id=peer(to), device_id_type=MESH,
        )

    half_x = (0, first_rows, OWN, OTHER_HALF)
    x_own = [(1 + n, later_rows, OWN, x) for n, x in enumerate(ACROSS)]
    x_first = [(4 + n, first_rows, OWN, x) for n, x in enumerate(ACROSS)]
    half_own = (7, later_rows, OWN, OTHER_HALF)
    half_on = [(8 + n, first_rows, OTHER_HALF, x) for n, x in enumerate(ACROSS)]
    x_on = [(11 + n, later_rows, x, OTHER_HALF) for n, x in enumerate(ACROSS)]

    def spread(number, rows_of, flip, to):
        copy = ag_copy(number, rows_of(flip), to)
        copy.start()
        waits.append(copy)

    def arrived(number, rows_of, flip, to):
        ag_copy(number, rows_of(plus(flip, to)), to).wait_recv()

    for message in (half_x, *x_own, *x_first, half_own):
        spread(*message)

    def last_copy(m, other):
        return pltpu.make_async_remote_copy(
            pf.at[pl.ds(ROWS, 8)], pf.at[pl.ds(ROWS, 8)], last_send.at[m], last_recv.at[0],
            device_id=peer(other), device_id_type=MESH,
        )

    @pl.when(is_last)
    def _():
        for m, other in enumerate(OTHERS):
            last_copy(m, other).start()

    faces(0, 5)
    arrived(*half_x)
    for n in range(3):
        spread(*half_on[n])
    for n in (1, 2, 0):
        arrived(*x_own[n])
        spread(*x_on[n])
    faces(5, 15)

    @pl.when(area < here.areas - 1)
    def _():
        row_copy(0, cond).wait_recv()
        row_copy(1, hh).wait_recv()

    @pl.when(area == here.areas - 1)
    def _():
        cond[:, pl.ds(ROWS, 8), :] = jnp.zeros((LAYERS, 8, COLS), jnp.float32)
        hh[:, pl.ds(ROWS, 8), :] = jnp.zeros((LAYERS, 8, COLS), jnp.float32)

    faces(15, 16)
    for message in (*x_first, half_own, *half_on, *x_on):
        arrived(*message)

    @pl.when(here.slab < 7)
    def _():
        last_copy(0, OTHERS[0]).wait_recv()

    for copy in waits:
        copy.wait_send()

    @pl.when(is_last)
    def _():
        for m, other in enumerate(OTHERS):
            last_copy(m, other).wait_send()

    @pl.when(here.slab > 0)
    def _():
        halo_up.wait_send()

    @pl.when(here.slab < 7)
    def _():
        halo_down.wait_send()

    @pl.when(is_first == False)
    def _():
        part_copy(0, 0).wait_send()

    @pl.when(is_last == False)
    def _():
        part_copy(0, 1).wait_send()

    @pl.when(area > 0)
    def _():
        row_copy(0, cond).wait_send()
        row_copy(1, hh).wait_send()

    @pl.when(crosses_up)
    def _():
        for copy in (forward_up, *to_up):
            copy.wait_send()

    @pl.when(crosses_down)
    def _():
        for copy in (forward_down, *to_down):
            copy.wait_send()


CHUNK = 64


def write_kernel(hh, hr, gr, hc, gc, pf, cell, rows_out, cols_out, cell_v, rows_v, cols_v, sems):
    chunks = ROWS // CHUNK

    def copies(i):
        rows = pl.ds(pl.multiple_of(i * CHUNK, 8), CHUNK)
        return [
            pltpu.make_async_copy(v.at[:, rows], o.at[:, rows], sems.at[n, i])
            for n, (v, o) in enumerate(((cell_v, cell), (rows_v, rows_out), (cols_v, cols_out)))
        ]

    @pl.loop(0, chunks)
    def _(i):
        start = pl.multiple_of(i * CHUNK, 8)
        rows = pl.ds(start, CHUNK)
        wide = pf[pl.ds(start, CHUNK + 8), :]
        pressure = wide[:CHUNK]
        row_drop = pressure - pltpu.roll(wide, CHUNK + 7, 0)[:CHUNK]
        col_drop = pressure - pltpu.roll(pressure, COLS - 1, 1)
        for k in range(LAYERS):
            cell_v[k, rows, :] = pressure + hh[k, rows, :]
            rows_v[k, rows, :] = hr[k, rows, :] * row_drop + gr[k, rows, :]
            cols_v[k, rows, :] = hc[k, rows, :] * col_drop + gc[k, rows, :]
        for copy in copies(i):
            copy.start()

    @pl.loop(0, chunks)
    def _(i):
        for copy in copies(i):
            copy.wait()


def local(permeability, mobility, thickness, caprock, plume, storage, source, pressure_old):
    f32, i32 = jnp.float32, jnp.int32
    vmem = pl.BlockSpec(memory_space=pltpu.VMEM)
    hbm = pl.BlockSpec(memory_space=pltpu.HBM)
    dma = pltpu.SemaphoreType.DMA
    V = pltpu.VMEM
    full = V((LAYERS, ROWS, COLS), f32)
    tall = V((LAYERS, ROWS + 8, COLS), f32)
    arrays = (permeability, mobility, thickness, caprock, plume, storage, source, pressure_old)
    arrays = [pltpu.with_memory_space_constraint(x, pltpu.HBM) for x in arrays]
    kept = pl.pallas_call(
        gather_kernel,
        out_shape=[tall, full, full, full, full, V((ROWS + 8, COLS), f32)],
        in_specs=[hbm] * 8,
        out_specs=[vmem] * 6,
        scratch_shapes=[
            V((LAYERS, ROWS, COLS), f32), V((LAYERS, ROWS, COLS), f32), V((LAYERS, ROWS + 8, COLS), f32),
            V((ROWS, COLS), i32), V((ROWS, COLS), i32), V((2, ROWS, COLS), f32),
            *[V((4, 2, r, COLS), f32) for r in PART_ROWS],
            *[V((2, 2, r, COLS), f32) for r in PART_ROWS],
            *[V((2, r, COLS), f32) for r in PART_ROWS],
            V((2, 2, LAYERS, 8, COLS), f32), V((2, 2, 8, COLS), i32), V((2, 8, COLS), f32),
            V((7, 8, COLS), f32), V((8, COLS), f32), V((2, 8, COLS), f32),
            V((2, WIDE, COLS), f32), V((2, WIDE, COLS), i32), V((3, WIDE, COLS), f32),
            pltpu.SMEM((LAYERS,), f32), V((8, 8, 128), f32), V((33, 8, 128), f32),
            *[V((WIDE, COLS), f32) for _ in range(5)],
            dma((8, 4)), dma((3, 5)), dma((1,)), dma((3, 7)), dma((3, 7)), dma((14,)), dma((14,)),
            dma((7,)), dma((7,)),
            dma((2, 4)), dma((2,)), dma((7,)), dma((1,)), dma((2,)), pltpu.SemaphoreType.REGULAR,
            dma((2,)), dma((2,)), dma((2, 5)), dma((2, 5)), dma((2,)), dma((2,)),
            dma((7,)), dma((1,)),
        ],
        compiler_params=pltpu.CompilerParams(
            collective_id=0, has_side_effects=True, vmem_limit_bytes=26 << 20
        ),
        name="gather",
    )(*arrays)
    return pl.pallas_call(
        write_kernel,
        out_shape=[jax.ShapeDtypeStruct((LAYERS, ROWS, COLS), f32)] * 3,
        in_specs=[vmem] * 6,
        out_specs=[hbm] * 3,
        scratch_shapes=[V((LAYERS, ROWS, COLS), f32)] * 3 + [dma((3, ROWS // CHUNK))],
        compiler_params=pltpu.CompilerParams(vmem_limit_bytes=16 << 20),
        name="write",
    )(*kept)


def solution(mesh):
    in_specs = (
        P("layer", "area", None),
        P("layer", "area", None),
        P("layer"),
        P("area", None),
        P("area", None),
        P("area", None),
        P("area", None),
        P("area", None),
    )
    out_specs = (P("layer", "area", None), P("layer", "area", None), P("layer", "area", None))
    return jax.shard_map(
        lambda *args: tuple(local(*args)), mesh=mesh, in_specs=in_specs, out_specs=out_specs, check_vma=False
    )
```

```python
import functools

import jax
import jax.numpy as jnp
from jax import lax
from jax.experimental import pallas as pl
from jax.experimental.pallas import tpu as pltpu
from jax.sharding import PartitionSpec as P

SWEEPS = 3
buoyancy_scale = 0.3
gravity_scale = 0.05
gas_density = 0.7
brine_density = 1.0

LAYERS = 4
ROWS = 512
COLS = 512
SLAB = 64
HALO = 8
WIDE = SLAB + 2 * HALO
MESH = pl.DeviceIdType.MESH

ORDERS = ((0, 1, 2), (1, 2, 0), (2, 0, 1))
PART_START = (0, 24, 48)
PART_ROWS = (24, 24, 16)
FLIPS = ((1, 1, 1), (1, 1, 0), (0, 1, 1), (1, 0, 1), (1, 0, 0), (0, 1, 0), (0, 0, 1), (0, 0, 0))
OTHERS = FLIPS[:-1]
X_FIRST = 24
ACROSS = ((1, 1, 0), (1, 0, 0), (0, 1, 0))
OTHER_HALF = (0, 0, 1)
OWN = (0, 0, 0)


def harmonic(near_value, far_value):
    summed = near_value + far_value
    divisor = jnp.where(summed > 0, summed, 1.0)
    return 2.0 * near_value * far_value / divisor


def flip_of(*dims):
    return tuple(1 if d in dims else 0 for d in range(3))


def plus(one, two):
    return tuple((a + b) % 2 for a, b in zip(one, two))


class Place:
    def __init__(self):
        self.area = lax.axis_index("area")
        self.layer = lax.axis_index("layer")
        self.areas = lax.axis_size("area")
        x = self.layer % 4
        second = x // 2
        first = (x % 2) + second - 2 * (x % 2) * second
        self.code = (first, second, self.layer // 4)
        self.parity = self.area % 2
        self.slab = self.slab_of((0, 0, 0))

    def flipped(self, flip):
        return tuple((1 - c) if f else c for c, f in zip(self.code, flip))

    def layer_of(self, flip):
        first, second, half = self.flipped(flip)
        x = 2 * second + first + second - 2 * first * second
        return half * 4 + x

    def slab_of(self, flip):
        first, second, half = self.flipped(flip)
        x = 2 * second + first + second - 2 * first * second
        order = x + half * (7 - 2 * x)
        return order + self.parity * (7 - 2 * order)

    def layer_of_slab(self, slab):
        order = slab + self.parity * (7 - 2 * slab)
        return order + (order // 4) * (11 - 2 * order)

    def rows(self, flip, start, count):
        return pl.ds(pl.multiple_of(self.slab_of(flip) * SLAB + start, 8), count)


def gather_kernel(
    perm, mob, thick, cap, plu, sto, src, old,
    hh, hr, gr, hc, gc, pf,
    permv, mobv, cond, capv, pluv, tb, r1a, r1b, r1c, r2a, r2b, r2c, r3a, r3b, r3c,
    edge_3d, edge_2d, tiles, parts, sums, cross,
    wide, edge_i, edge_f, thick_s, thick_all, table, gas, t_row, t_col, right_hand, inverse,
    in_sem, edge_sem, thick_sem, rs_send, rs_recv, ag_send, ag_recv, th_send, th_recv,
    part_load, part_send, part_recv, sum_send, sum_recv, ready,
    halo_send, halo_recv, input_send, input_recv, row_send, row_recv, last_send, last_recv,
):
    here = Place()
    area, layer = here.area, here.layer
    r1, r2, r3 = (r1a, r1b, r1c), (r2a, r2b, r2c), (r3a, r3b, r3c)
    waits = []
    is_first = here.slab == 0
    is_last = here.slab == 7

    def peer(flip):
        return (area, here.layer_of(flip))

    loads = []
    thick_copy = pltpu.make_async_copy(thick, thick_s, thick_sem.at[0])
    thick_copy.start()
    part_copies = []
    for side, first_row in ((0, 0), (1, ROWS - HALO)):
        rows = pl.ds(first_row, HALO)
        part_copies += [
            pltpu.make_async_copy(cap.at[rows], edge_2d.at[0, side], part_load.at[side, 0]),
            pltpu.make_async_copy(plu.at[rows], edge_2d.at[1, side], part_load.at[side, 1]),
            pltpu.make_async_copy(perm.at[:, rows], edge_3d.at[0, side], part_load.at[side, 2]),
            pltpu.make_async_copy(mob.at[:, rows], edge_3d.at[1, side], part_load.at[side, 3]),
        ]
    for copy in part_copies:
        copy.start()
    for n, flip in enumerate(FLIPS):
        rows = here.rows(flip, 0, SLAB)
        group = [
            pltpu.make_async_copy(cap.at[rows], capv.at[rows], in_sem.at[n, 0]),
            pltpu.make_async_copy(plu.at[rows], pluv.at[rows], in_sem.at[n, 1]),
            pltpu.make_async_copy(perm.at[:, rows], permv.at[:, rows], in_sem.at[n, 2]),
            pltpu.make_async_copy(mob.at[:, rows], mobv.at[:, rows], in_sem.at[n, 3]),
        ]
        for copy in group:
            copy.start()
        loads.append(group)

    barrier = pltpu.get_barrier_semaphore()
    for flip in OTHERS:
        pl.semaphore_signal(barrier, inc=1, device_id=peer(flip), device_id_type=MESH)
    both_sides = [((area + step) % here.areas, layer) for step in (1, here.areas - 1)]

    @pl.when(here.parity == 0)
    def _():
        for neighbour in both_sides:
            pl.semaphore_signal(barrier, inc=1, device_id=neighbour, device_id_type=MESH)

    base = here.slab * SLAB
    sources = (cap, plu, sto, src, old)
    targets = (edge_i.at[0], edge_i.at[1], edge_f.at[0], edge_f.at[1], edge_f.at[2])

    def edge_copies(sem_row, first_row, count, at):
        rows = pl.ds(pl.multiple_of(base + first_row, 8), count)
        return [
            pltpu.make_async_copy(s.at[rows], t.at[pl.ds(at, count)], edge_sem.at[sem_row, n])
            for n, (s, t) in enumerate(zip(sources, targets))
        ]

    mid_copies = edge_copies(0, 0, SLAB, HALO)
    for copy in mid_copies:
        copy.start()

    @pl.when(here.slab > 0)
    def _():
        for copy in edge_copies(1, -HALO, HALO, 0):
            copy.start()

    @pl.when(here.slab < 7)
    def _():
        for copy in edge_copies(2, SLAB, HALO, HALO + SLAB):
            copy.start()

    thick_copy.wait()
    sublane = lax.broadcasted_iota(jnp.int32, (8, 128), 0)
    tile = jnp.zeros((8, 128), jnp.float32)
    for k in range(LAYERS):
        tile = jnp.where(sublane == k, thick_s[k], tile)
    thick_all[layer] = tile

    def input_sends():
        up = [
            pltpu.make_async_remote_copy(
                s.at[pl.ds(0, HALO)], t.at[pl.ds(HALO + SLAB, HALO)],
                input_send.at[0, n], input_recv.at[0, n],
                device_id=(area - 1, layer), device_id_type=MESH,
            )
            for n, (s, t) in enumerate(zip(sources, targets))
        ]
        down = [
            pltpu.make_async_remote_copy(
                s.at[pl.ds(ROWS - HALO, HALO)], t.at[pl.ds(0, HALO)],
                input_send.at[1, n], input_recv.at[1, n],
                device_id=(area + 1, layer), device_id_type=MESH,
            )
            for n, (s, t) in enumerate(zip(sources, targets))
        ]
        return up, down

    to_up, to_down = input_sends()
    crosses_up = is_first & (area > 0)
    crosses_down = is_last & (area < here.areas - 1)
    top_edge = is_first & (area == 0)
    bottom_edge = is_last & (area == here.areas - 1)

    sub8 = lax.broadcasted_iota(jnp.int32, (8, COLS), 0)
    for copy in part_copies:
        copy.wait()
    for side in (0, 1):
        top = edge_2d[0, side]
        bottom = edge_2d[1, side]
        trans = buoy = jnp.zeros((8, COLS), jnp.float32)
        for k in range(LAYERS):
            depth = layer * LAYERS + k
            flow = edge_3d[0, side, k] * edge_3d[1, side, k] * thick_s[k]
            flow = jnp.where(depth >= top, flow, 0.0)
            trans = trans + flow
            buoy = buoy + jnp.where(depth < bottom, flow, 0.0)
        used = (sub8 < 4) if side == 0 else (sub8 >= 4)
        tiles[side] = jnp.where(used, trans, pltpu.roll(buoy, 4, 0))

    pl.semaphore_wait(barrier, 7 + 2 * here.parity)

    @pl.when(here.parity == 1)
    def _():
        for neighbour in both_sides:
            pl.semaphore_signal(ready, inc=1, device_id=neighbour, device_id_type=MESH)

    def part_copy(m, side):
        return pltpu.make_async_remote_copy(
            tiles.at[side], parts.at[m], part_send.at[side], part_recv.at[m],
            device_id=peer(OTHERS[m]), device_id_type=MESH,
        )

    for m, other in enumerate(OTHERS):
        for side, owner in ((0, 0), (1, 7)):

            @pl.when(here.slab_of(other) == owner)
            def _(m=m, side=side):
                part_copy(m, side).start()

    for m, other in enumerate(OTHERS):
        copy = pltpu.make_async_remote_copy(
            thick_all.at[layer], thick_all.at[layer], th_send.at[m], th_recv.at[m],
            device_id=peer(other), device_id_type=MESH,
        )
        copy.start()
        waits.append(copy)

    def conduct_slab(n, flip):
        for copy in loads[n]:
            copy.wait()
        start = here.slab_of(flip) * SLAB

        @pl.loop(0, SLAB // 8)
        def _(i):
            rows = pl.ds(pl.multiple_of(start + i * 8, 8), 8)
            top = capv[rows, :]
            bottom = pluv[rows, :]
            trans = None
            for k in range(LAYERS):
                depth = layer * LAYERS + k
                flow = permv[k, rows, :] * mobv[k, rows, :] * thick_s[k]
                flow = jnp.where(depth >= top, flow, 0.0)
                cond[k, rows, :] = flow
                part = jnp.where(depth < bottom, flow, 0.0)
                trans, buoy = (flow, part) if trans is None else (trans + flow, buoy + part)
            tb[0, rows, :] = trans
            tb[1, rows, :] = buoy

    def rs_copy(q, number, rows, buffer, dim):
        return pltpu.make_async_remote_copy(
            tb.at[:, rows], buffer, rs_send.at[q, number], rs_recv.at[q, number],
            device_id=peer(flip_of(dim)), device_id_type=MESH,
        )

    PIECES = ((1, 1), (1, 0), (0, 1), (0, 0))

    def part_rows(q, flip):
        return here.rows(flip, PART_START[q], PART_ROWS[q])

    def first_copy(q, n):
        d1, d2, d3 = ORDERS[q]
        e2, e3 = PIECES[n]
        flip = flip_of(*([d1] + [d2] * e2 + [d3] * e3))
        return flip, rs_copy(q, n, part_rows(q, flip), r1[q].at[n], d1)

    def second_copy(q, n):
        d1, d2, d3 = ORDERS[q]
        flip = flip_of(*([d2] + ([d3] if n == 0 else [])))
        return flip, rs_copy(q, 4 + n, part_rows(q, flip), r2[q].at[n], d2)

    def third_copy(q):
        d1, d2, d3 = ORDERS[q]
        flip = flip_of(d3)
        return flip, rs_copy(q, 6, part_rows(q, flip), r3[q], d3)

    held = []
    for n, flip in enumerate(FLIPS):
        conduct_slab(n, flip)
        for q in range(3):
            for m in range(4):
                owner, copy = first_copy(q, m)
                if owner == flip:
                    waits.append(copy)
                    if m == 3:
                        held.append(copy)
                    else:
                        copy.start()

    def row_copy(n, array):
        return pltpu.make_async_remote_copy(
            array.at[:, pl.ds(0, 8)], array.at[:, pl.ds(ROWS, 8)], row_send.at[n], row_recv.at[n],
            device_id=(area - 1, layer), device_id_type=MESH,
        )

    def across(tile):
        return jnp.concatenate([tile] * (COLS // 128), axis=1)

    def gas_sum(blocks, top, bottom):
        def lookup(index, count):
            def step(block, found):
                for k in range(LAYERS):
                    depth = block * LAYERS + k
                    found = jnp.where(depth < index, across(table[depth + 1]), found)
                return found

            return lax.fori_loop(0, count, step, jnp.zeros(index.shape, jnp.float32))

        return jnp.maximum(lookup(bottom, blocks) - lookup(top, jnp.minimum(blocks, 4)), 0.0)

    def heads(low, high):
        @pl.loop(low, high)
        def _(i):
            rows = pl.ds(pl.multiple_of(i * 8, 8), 8)
            top = capv[rows, :]
            bottom = pluv[rows, :]
            above = across(table[layer * LAYERS]) - (brine_density - gas_density) * gas_sum(layer, top, bottom)
            for k in range(LAYERS):
                depth = layer * LAYERS + k
                inside = (depth >= top) & (depth < bottom)
                mass = jnp.where(inside, gas_density * thick_s[k], brine_density * thick_s[k])
                hh[k, rows, :] = gravity_scale * (above + 0.5 * mass)
                above = above + mass

    lane_last = lax.broadcasted_iota(jnp.int32, (32, COLS), 1) < COLS - 1

    def faces(low, high):
        @pl.loop(low * LAYERS, high * LAYERS)
        def _(i):
            k = i % LAYERS
            start = pl.multiple_of((i // LAYERS) * 32, 8)
            flow = cond[k, pl.ds(start, 40), :]
            head = hh[k, pl.ds(start, 40), :]
            next_flow = pltpu.roll(flow, 39, 0)[:32]
            next_head = pltpu.roll(head, 39, 0)[:32]
            flow = flow[:32]
            head = head[:32]
            rows = pl.ds(start, 32)
            face = harmonic(flow, next_flow)
            hr[k, rows, :] = face
            gr[k, rows, :] = face * (head - next_head)
            side_flow = jnp.where(lane_last, pltpu.roll(flow, COLS - 1, 1), 0.0)
            side_head = pltpu.roll(head, COLS - 1, 1)
            face = harmonic(flow, side_flow)
            hc[k, rows, :] = face
            gc[k, rows, :] = face * (head - side_head)

    def second(n):
        for q in range(3):
            _, arrived = first_copy(q, n)
            arrived.wait_recv()
            flip, copy = second_copy(q, n)
            rows = part_rows(q, flip)
            tb[:, rows, :] = tb[:, rows, :] + r1[q][n]
            copy.start()
            waits.append(copy)

    forward_up = pltpu.make_async_remote_copy(
        sums, cross.at[1], sum_send.at[0], sum_recv.at[1],
        device_id=(area - 1, layer), device_id_type=MESH,
    )
    forward_down = pltpu.make_async_remote_copy(
        sums, cross.at[0], sum_send.at[0], sum_recv.at[0],
        device_id=(area + 1, layer), device_id_type=MESH,
    )

    def forward_edges():
        for ends, side in ((is_first, 0), (is_last, 1)):

            @pl.when(ends)
            def _(side=side):
                for m in range(7):
                    part_copy(m, side).wait_recv()
                total = tiles[side]
                for m in range(7):
                    total = total + parts[m]
                sums[...] = total

        @pl.when(crosses_up)
        def _():
            for copy in (forward_up, *to_up):
                copy.start()

        @pl.when(crosses_down)
        def _():
            for copy in (forward_down, *to_down):
                copy.start()

        @pl.when(area > 0)
        def _():
            row_copy(0, cond).start()

    def gas_rows(at):
        rows = pl.ds(at, 8)
        gas[rows, :] = buoyancy_scale * gas_sum(8, edge_i[0, rows, :], edge_i[1, rows, :])

    second(0)
    for copy in held:
        copy.start()

    second(1)

    for m, other in enumerate(OTHERS):
        pltpu.make_async_remote_copy(
            thick_all.at[layer], thick_all.at[here.layer_of(other)], th_send.at[m], th_recv.at[m],
            device_id=peer(other), device_id_type=MESH,
        ).wait_recv()
    total = jnp.zeros((8, 128), jnp.float32)
    table[0] = total
    for block in range(8):
        for k in range(LAYERS):
            total = total + jnp.broadcast_to(thick_all[block, pl.ds(k, 1), :], (8, 128))
            table[block * LAYERS + k + 1] = total


    @pl.when(here.parity == 1)
    def _():
        forward_edges()

    heads(0, 32)

    @pl.when(here.parity == 0)
    def _():
        pl.semaphore_wait(ready, 2)
        forward_edges()

    for copy in mid_copies:
        copy.wait()

    @pl.when(here.slab > 0)
    def _():
        for copy in edge_copies(1, -HALO, HALO, 0):
            copy.wait()

    @pl.when(here.slab < 7)
    def _():
        for copy in edge_copies(2, SLAB, HALO, HALO + SLAB):
            copy.wait()

    for q in range(3):
        first_copy(q, 2)[1].wait_recv()
        second_copy(q, 0)[1].wait_recv()
        flip, copy = third_copy(q)
        rows = part_rows(q, flip)
        tb[:, rows, :] = tb[:, rows, :] + (r1[q][2] + r2[q][0])
        copy.start()
        waits.append(copy)

    heads(32, 64)

    @pl.when(area > 0)
    def _():
        row_copy(1, hh).start()

    @pl.loop(1, WIDE // 8 - 1)
    def _(i):
        gas_rows(pl.multiple_of(i * 8, 8))

    for q in range(3):
        first_copy(q, 3)[1].wait_recv()
        second_copy(q, 1)[1].wait_recv()
        third_copy(q)[1].wait_recv()
        mine = part_rows(q, (0, 0, 0))
        at = pl.ds(HALO + PART_START[q], PART_ROWS[q])
        wide[:, at, :] = tb[:, mine, :] + r1[q][3] + (r2[q][1] + r3[q][...])

    up_layer = here.layer_of_slab(jnp.maximum(here.slab - 1, 0))
    down_layer = here.layer_of_slab(jnp.minimum(here.slab + 1, 7))
    halo_up = pltpu.make_async_remote_copy(
        wide.at[:, pl.ds(HALO, HALO)], wide.at[:, pl.ds(HALO + SLAB, HALO)],
        halo_send.at[0], halo_recv.at[0], device_id=(area, up_layer), device_id_type=MESH,
    )
    halo_down = pltpu.make_async_remote_copy(
        wide.at[:, pl.ds(SLAB, HALO)], wide.at[:, pl.ds(0, HALO)],
        halo_send.at[1], halo_recv.at[1], device_id=(area, down_layer), device_id_type=MESH,
    )

    @pl.when(here.slab > 0)
    def _():
        halo_up.start()

    @pl.when(here.slab < 7)
    def _():
        halo_down.start()

    def blank(at):
        rows = pl.ds(at, HALO)
        edge_i[:, rows, :] = jnp.zeros((2, HALO, COLS), jnp.int32)
        edge_f[0, rows, :] = jnp.ones((HALO, COLS), jnp.float32)
        edge_f[1, rows, :] = jnp.zeros((HALO, COLS), jnp.float32)
        edge_f[2, rows, :] = jnp.zeros((HALO, COLS), jnp.float32)
        wide[:, rows, :] = jnp.zeros((2, HALO, COLS), jnp.float32)

    def unpack(slot, at, used):
        rows = pl.ds(at, HALO)
        tile = cross[slot]
        wide[0, rows, :] = jnp.where(used, tile, 0.0)
        wide[1, rows, :] = jnp.where(used, pltpu.roll(tile, 4, 0), 0.0)

    @pl.when(top_edge)
    def _():
        blank(0)

    @pl.when(bottom_edge)
    def _():
        blank(HALO + SLAB)

    @pl.when(crosses_up)
    def _():
        for copy in (forward_down, *to_down):
            copy.wait_recv()
        unpack(0, 0, sub8 >= 4)

    @pl.when(crosses_down)
    def _():
        for copy in (forward_up, *to_up):
            copy.wait_recv()
        unpack(1, HALO + SLAB, sub8 < 4)

    gas_rows(0)
    gas_rows(HALO + SLAB)

    @pl.when(here.slab > 0)
    def _():
        halo_down.wait_recv()

    @pl.when(here.slab < 7)
    def _():
        halo_up.wait_recv()

    lane = lax.broadcasted_iota(jnp.int32, (WIDE, COLS), 1)

    def after(x):
        return pltpu.roll(x, WIDE - 1, 0)

    def before(x):
        return pltpu.roll(x, 1, 0)

    def right(x):
        return jnp.where(lane < COLS - 1, pltpu.roll(x, COLS - 1, 1), 0.0)

    def left(x):
        return jnp.where(lane > 0, pltpu.roll(x, 1, 1), 0.0)

    trans = wide[0]
    face_row = harmonic(trans, after(trans))
    t_row[...] = face_row
    face_col = harmonic(trans, right(trans))
    t_col[...] = face_col
    diagonal = edge_f[0] + face_row + before(face_row) + face_col + left(face_col)
    inverse[...] = 1.0 / diagonal
    buoy = wide[1]
    drive = gas[...]
    push = harmonic(buoy, after(buoy)) * (after(drive) - drive)
    total = push - before(push)
    push = harmonic(buoy, right(buoy)) * (right(drive) - drive)
    total = total + (push - left(push))
    right_hand[...] = edge_f[0] * edge_f[2] + edge_f[1] + total

    for sweep in range(SWEEPS):
        pressure = edge_f[2]
        face_row = t_row[...]
        face_col = t_col[...]
        inflow = face_row * after(pressure) + before(face_row * pressure)
        inflow = inflow + (face_col * right(pressure) + left(face_col * pressure))
        edge_f[2] = (right_hand[...] + inflow) * inverse[...]

    pf[here.rows((0, 0, 0), 0, SLAB), :] = edge_f[2, pl.ds(HALO, SLAB), :]

    @pl.when(is_last)
    def _():
        pf[pl.ds(ROWS, 8), :] = edge_f[2, pl.ds(HALO + SLAB, 8), :]

    def first_rows(flip):
        return here.rows(flip, 0, X_FIRST)

    def later_rows(flip):
        return here.rows(flip, X_FIRST, SLAB - X_FIRST)

    def ag_copy(number, rows, to):
        return pltpu.make_async_remote_copy(
            pf.at[rows], pf.at[rows], ag_send.at[number], ag_recv.at[number],
            device_id=peer(to), device_id_type=MESH,
        )

    half_x = (0, first_rows, OWN, OTHER_HALF)
    x_own = [(1 + n, later_rows, OWN, x) for n, x in enumerate(ACROSS)]
    x_first = [(4 + n, first_rows, OWN, x) for n, x in enumerate(ACROSS)]
    half_own = (7, later_rows, OWN, OTHER_HALF)
    half_on = [(8 + n, first_rows, OTHER_HALF, x) for n, x in enumerate(ACROSS)]
    x_on = [(11 + n, later_rows, x, OTHER_HALF) for n, x in enumerate(ACROSS)]

    def spread(number, rows_of, flip, to):
        copy = ag_copy(number, rows_of(flip), to)
        copy.start()
        waits.append(copy)

    def arrived(number, rows_of, flip, to):
        ag_copy(number, rows_of(plus(flip, to)), to).wait_recv()

    for message in (half_x, *x_own, *x_first, half_own):
        spread(*message)

    def last_copy(m, other):
        return pltpu.make_async_remote_copy(
            pf.at[pl.ds(ROWS, 8)], pf.at[pl.ds(ROWS, 8)], last_send.at[m], last_recv.at[0],
            device_id=peer(other), device_id_type=MESH,
        )

    @pl.when(is_last)
    def _():
        for m, other in enumerate(OTHERS):
            last_copy(m, other).start()

    faces(0, 5)
    arrived(*half_x)
    for n in range(3):
        spread(*half_on[n])
    for n in (1, 2, 0):
        arrived(*x_own[n])
        spread(*x_on[n])
    faces(5, 15)

    @pl.when(area < here.areas - 1)
    def _():
        row_copy(0, cond).wait_recv()
        row_copy(1, hh).wait_recv()

    @pl.when(area == here.areas - 1)
    def _():
        cond[:, pl.ds(ROWS, 8), :] = jnp.zeros((LAYERS, 8, COLS), jnp.float32)
        hh[:, pl.ds(ROWS, 8), :] = jnp.zeros((LAYERS, 8, COLS), jnp.float32)

    faces(15, 16)
    for message in (*x_first, half_own, *half_on, *x_on):
        arrived(*message)

    @pl.when(here.slab < 7)
    def _():
        last_copy(0, OTHERS[0]).wait_recv()

    for copy in waits:
        copy.wait_send()

    @pl.when(is_last)
    def _():
        for m, other in enumerate(OTHERS):
            last_copy(m, other).wait_send()

    @pl.when(here.slab > 0)
    def _():
        halo_up.wait_send()

    @pl.when(here.slab < 7)
    def _():
        halo_down.wait_send()

    @pl.when(is_first == False)
    def _():
        part_copy(0, 0).wait_send()

    @pl.when(is_last == False)
    def _():
        part_copy(0, 1).wait_send()

    @pl.when(area > 0)
    def _():
        row_copy(0, cond).wait_send()
        row_copy(1, hh).wait_send()

    @pl.when(crosses_up)
    def _():
        for copy in (forward_up, *to_up):
            copy.wait_send()

    @pl.when(crosses_down)
    def _():
        for copy in (forward_down, *to_down):
            copy.wait_send()


CHUNK = 64


def write_kernel(hh, hr, gr, hc, gc, pf, cell, rows_out, cols_out, cell_v, rows_v, cols_v, sems):
    chunks = ROWS // CHUNK

    def copies(i):
        rows = pl.ds(pl.multiple_of(i * CHUNK, 8), CHUNK)
        return [
            pltpu.make_async_copy(v.at[:, rows], o.at[:, rows], sems.at[n, i])
            for n, (v, o) in enumerate(((cell_v, cell), (rows_v, rows_out), (cols_v, cols_out)))
        ]

    @pl.loop(0, chunks)
    def _(i):
        start = pl.multiple_of(i * CHUNK, 8)
        rows = pl.ds(start, CHUNK)
        wide = pf[pl.ds(start, CHUNK + 8), :]
        pressure = wide[:CHUNK]
        row_drop = pressure - pltpu.roll(wide, CHUNK + 7, 0)[:CHUNK]
        col_drop = pressure - pltpu.roll(pressure, COLS - 1, 1)
        for k in range(LAYERS):
            cell_v[k, rows, :] = pressure + hh[k, rows, :]
            rows_v[k, rows, :] = hr[k, rows, :] * row_drop + gr[k, rows, :]
            cols_v[k, rows, :] = hc[k, rows, :] * col_drop + gc[k, rows, :]
        for copy in copies(i):
            copy.start()

    @pl.loop(0, chunks)
    def _(i):
        for copy in copies(i):
            copy.wait()


def local(permeability, mobility, thickness, caprock, plume, storage, source, pressure_old):
    f32, i32 = jnp.float32, jnp.int32
    vmem = pl.BlockSpec(memory_space=pltpu.VMEM)
    hbm = pl.BlockSpec(memory_space=pltpu.HBM)
    dma = pltpu.SemaphoreType.DMA
    V = pltpu.VMEM
    full = V((LAYERS, ROWS, COLS), f32)
    tall = V((LAYERS, ROWS + 8, COLS), f32)
    arrays = (permeability, mobility, thickness, caprock, plume, storage, source, pressure_old)
    arrays = [pltpu.with_memory_space_constraint(x, pltpu.HBM) for x in arrays]
    kept = pl.pallas_call(
        gather_kernel,
        out_shape=[tall, full, full, full, full, V((ROWS + 8, COLS), f32)],
        in_specs=[hbm] * 8,
        out_specs=[vmem] * 6,
        scratch_shapes=[
            V((LAYERS, ROWS, COLS), f32), V((LAYERS, ROWS, COLS), f32), V((LAYERS, ROWS + 8, COLS), f32),
            V((ROWS, COLS), i32), V((ROWS, COLS), i32), V((2, ROWS, COLS), f32),
            *[V((4, 2, r, COLS), f32) for r in PART_ROWS],
            *[V((2, 2, r, COLS), f32) for r in PART_ROWS],
            *[V((2, r, COLS), f32) for r in PART_ROWS],
            V((2, 2, LAYERS, 8, COLS), f32), V((2, 2, 8, COLS), i32), V((2, 8, COLS), f32),
            V((7, 8, COLS), f32), V((8, COLS), f32), V((2, 8, COLS), f32),
            V((2, WIDE, COLS), f32), V((2, WIDE, COLS), i32), V((3, WIDE, COLS), f32),
            pltpu.SMEM((LAYERS,), f32), V((8, 8, 128), f32), V((33, 8, 128), f32),
            *[V((WIDE, COLS), f32) for _ in range(5)],
            dma((8, 4)), dma((3, 5)), dma((1,)), dma((3, 7)), dma((3, 7)), dma((14,)), dma((14,)),
            dma((7,)), dma((7,)),
            dma((2, 4)), dma((2,)), dma((7,)), dma((1,)), dma((2,)), pltpu.SemaphoreType.REGULAR,
            dma((2,)), dma((2,)), dma((2, 5)), dma((2, 5)), dma((2,)), dma((2,)),
            dma((7,)), dma((1,)),
        ],
        compiler_params=pltpu.CompilerParams(
            collective_id=0, has_side_effects=True, vmem_limit_bytes=26 << 20
        ),
        name="gather",
    )(*arrays)
    return pl.pallas_call(
        write_kernel,
        out_shape=[jax.ShapeDtypeStruct((LAYERS, ROWS, COLS), f32)] * 3,
        in_specs=[vmem] * 6,
        out_specs=[hbm] * 3,
        scratch_shapes=[V((LAYERS, ROWS, COLS), f32)] * 3 + [dma((3, ROWS // CHUNK))],
        compiler_params=pltpu.CompilerParams(vmem_limit_bytes=16 << 20),
        name="write",
    )(*kept)


def solution(mesh):
    in_specs = (
        P("layer", "area", None),
        P("layer", "area", None),
        P("layer"),
        P("area", None),
        P("area", None),
        P("area", None),
        P("area", None),
        P("area", None),
    )
    out_specs = (P("layer", "area", None), P("layer", "area", None), P("layer", "area", None))
    return jax.shard_map(
        lambda *args: tuple(local(*args)), mesh=mesh, in_specs=in_specs, out_specs=out_specs, check_vma=False
    )
```
